32 devices in a mesh: groups: 2 (over x), wide: 16 (over z, y, core).
Axes of the slice: x: 2, y: 2, z: 4, core: 2. Of those that a mesh axis runs over, the one named last changes fastest.
Arguments:
- half_integrals: float32 [256, 512, 800], P(('groups', 'wide')), parts along dimension 0, may hold values from -40 to 40
- pair_list: int32 [256, 2], P('groups'), parts along dimension 0, may hold values from 0 to 199, as said below
- occupied_energy: float32 [400], P('groups'), parts along dimension 0, may hold values from -3 to -0.3
- virtual_orbitals: float32 [1600, 600], P('groups'), parts along dimension 0, may hold values from -0.21875 to 0.21875
- tile_order: int32 [64], replicated, may hold values from 0 to 63, each once
Outputs:
- transformed: float32 [256, 512, 600], P('groups', 'wide'), parts along dimension 0
- pair_rms: float32 [256], P('groups'), parts along dimension 0
The draws below stay inside these ranges and needn't reach their ends.
There are 2 independent parts, one for each index of `groups`. The reference program is written for one: setup_inputs(seed, part) draws one part's arguments, and reference() takes and returns one part's arrays. A program takes and returns all parts, laid end to end along the dimension named above; an argument that names none is the same for every part. Nothing has to cross between parts.
Inputs may be any that keep to these rules, and one draw needn't show every extreme that they name: `pair_list`: each row is a distinct pair (i, j) with i <= j.
All inputs are finite; a program needn't handle non-finite values.
Results may differ from the reference program's by a relative error of at most 0.00007.
Values sent between devices are 32-bit elements; how exact they have to be, the bound alone decides.
A program may use at most 128 MiB of HBM per device.

```python
import jax
import jax.numpy as jnp
from jax import lax

NOCC = 200
NBAS = 800
NVIRT = 600
S_WIN = 512
TILE_S = 8
PAIRS = 128
TILES = 64


def draw_half_integrals(key, part):
    scale_key = jax.random.fold_in(key, 11)
    base_key = jax.random.fold_in(key, 12)
    column_scale = jnp.exp(jax.random.uniform(scale_key, (S_WIN,), jnp.float32, jnp.log(0.3), jnp.log(3.0)))
    base = jnp.clip(jax.random.normal(base_key, (PAIRS, S_WIN, NBAS), jnp.float32), -6.0, 6.0)
    return (base * column_scale[None, :, None]).astype(jnp.float32)


def draw_pair_list(key, part):
    total = NOCC * (NOCC + 1) // 2
    chosen = jax.random.permutation(jax.random.fold_in(key, 21), total)[:PAIRS].astype(jnp.int32)
    orbital = jnp.arange(NOCC, dtype=jnp.int32)
    triangle = orbital * (orbital + 1) // 2
    second = jnp.sum((triangle[None, :] <= chosen[:, None]).astype(jnp.int32), axis=1) - 1
    first = chosen - jnp.take(triangle, second)
    return jnp.stack([first, second], axis=1).astype(jnp.int32)


def normal_values(own_key, shape, width, most, kind=jnp.bfloat16):
    values = jax.random.normal(own_key, shape, jnp.float32) * width
    return jnp.minimum(jnp.maximum(values, -most), most).astype(kind)


def setup_inputs(seed: int = 0, part: int = 0) -> dict:
    keys = jax.random.split(jax.random.key(seed), 6)
    part_keys = jax.random.split(jax.random.fold_in(keys[5], part), 6)
    return {
        "half_integrals": draw_half_integrals(jax.random.fold_in(jax.random.fold_in(keys[5], part), 71), part),
        "pair_list": draw_pair_list(jax.random.fold_in(jax.random.fold_in(keys[5], part), 71), part),
        "occupied_energy": jnp.clip(jax.random.uniform(part_keys[2], (NOCC,), jnp.float32, -3.0, -0.3), -3.0, -0.3),
        "virtual_orbitals": normal_values(part_keys[3], (NBAS, NVIRT), NBAS ** -0.5, 0.21875, jnp.float32),
        "tile_order": jax.random.permutation(keys[4], TILES).astype(jnp.int32),
    }


def reference(half_integrals, pair_list, occupied_energy, virtual_orbitals, tile_order):
    energy_sum = occupied_energy[pair_list[:, 0]] + occupied_energy[pair_list[:, 1]]
    weights = jnp.exp(0.3 * energy_sum).astype(jnp.float32)
    pair_count = half_integrals.shape[0]
    tiled = half_integrals.reshape(pair_count, TILES, TILE_S, NBAS)
    ordered = jnp.take(tiled, tile_order, axis=1).reshape(pair_count, S_WIN, NBAS)
    product = jnp.einsum('psr,ra->psa', ordered, virtual_orbitals, precision=lax.Precision.HIGHEST)
    transformed = product * weights[:, None, None]
    squares = lax.optimization_barrier(jnp.sum(transformed * transformed, axis=(1, 2)))
    pair_rms = jnp.sqrt(squares / (S_WIN * NVIRT) + 1e-06)
    return (transformed, pair_rms)
```

```python
import functools

import jax
import jax.numpy as jnp
from jax import lax
from jax.experimental import pallas as pl
from jax.experimental.pallas import tpu as pltpu
from jax.sharding import PartitionSpec as P

TILE_S = 8
LANES = 128
MESH = pl.DeviceIdType.MESH


def round_up(value, step):
    return (value + step - 1) // step * step


def split(value):
    high = value.astype(jnp.bfloat16)
    low = (value - high.astype(jnp.float32)).astype(jnp.bfloat16)
    return high, low


def prepare_kernel(
    order_ref, pair_ref, energy_ref, x_ref, w_ref, xs, w_high, w_low, scales,
    index_buf, turned, slot_of, sems,
):
    me = lax.axis_index("wide")
    step = pl.program_id(0)
    steps = pl.num_programs(0)
    pair_rows, basis, _ = x_ref.shape
    virtuals = w_ref.shape[1]
    deep = xs.shape[0]
    block_rows = TILE_S * pair_rows
    tiles = LANES // TILE_S
    side = lax.rem(step, 2)

    @pl.when(step == 0)
    def _():
        def invert(k, carry):
            slot_of[order_ref[k]] = k
            return carry

        lax.fori_loop(0, order_ref.shape[0], invert, 0)
        w_high[...] = jnp.zeros_like(w_high)
        w_low[...] = jnp.zeros_like(w_low)
        high, low = split(w_ref[...])
        w_high[:basis, :virtuals] = high
        w_low[:basis, :virtuals] = low
        my_rows = pl.ds(pl.multiple_of(me * pair_rows, pair_rows), pair_rows)
        orbitals = energy_ref.shape[1]
        orbital = lax.broadcasted_iota(jnp.int32, (pair_rows, orbitals), 1).astype(jnp.float32)
        energy = jnp.zeros((pair_rows, 1), jnp.float32)
        for k in range(2):
            line = pair_ref[k : k + 1, :].astype(jnp.float32)
            index_buf[...] = jnp.broadcast_to(line, (LANES, line.shape[1])).T
            hit = index_buf[my_rows, 0:1] == orbital
            energy = energy + jnp.sum(jnp.where(hit, energy_ref[...], 0.0), axis=1, keepdims=True)
        scales[...] = jnp.broadcast_to(jnp.exp(0.3 * energy), scales.shape)

    def copy(at, which, u):
        rows = pl.ds(pl.multiple_of(slot_of[at * tiles + u] * block_rows, block_rows), block_rows)
        return pltpu.make_async_copy(
            turned.at[which, :, pl.ds(u * block_rows, block_rows), :], xs.at[:, rows, :], sems.at[which, u]
        )

    @pl.when(step >= 2)
    def _():
        for u in range(tiles):
            copy(step - 2, side, u).wait()

    for p in range(pair_rows):
        for k in range(deep):
            size = min(LANES, basis - k * LANES)
            piece = x_ref[p, k * LANES : k * LANES + size, :]
            if size < LANES:
                piece = jnp.concatenate([piece, jnp.zeros((LANES - size, LANES), jnp.float32)], axis=0)
            turned[side, k, pl.ds(p, LANES, stride=pair_rows), :] = piece.T
    for u in range(tiles):
        copy(step, side, u).start()

    @pl.when(step == steps - 1)
    def _():
        for u in range(tiles):
            copy(step - 1, 1 - side, u).wait()
        for u in range(tiles):
            copy(step, side, u).wait()


def exchange_kernel(
    n, xs, w_high, w_low, scales, recv_main, recv_rest, sq_recv,
    x_buf, x_high, x_low, squares, sq_send, send_main, send_rest,
    x_sems, main_sems, rest_sems, main_recv_sems, rest_recv_sems,
    sq_sems, sq_recv_sems, own_sems,
):
    me = lax.axis_index("wide")
    _, span, pair_rows, full = send_main.shape
    rest = send_rest.shape[2] // span
    rows = span * pair_rows
    deep = xs.shape[0]
    plane = n // 4
    my_rows = pl.ds(pl.multiple_of(me * pair_rows, pair_rows), pair_rows)

    barrier = pltpu.get_barrier_semaphore()

    def greet(j, carry):
        pl.semaphore_signal(barrier, inc=1, device_id={"wide": lax.rem(me + j, n)}, device_id_type=MESH)
        return carry

    lax.fori_loop(1, n, greet, 0)

    sign = 1 - 2 * (me // (n // 2))
    my_plane = me // plane
    inner = jnp.minimum(my_plane, 3 - my_plane)

    def place(c):
        rank = c // plane
        away = 3 - rank - inner * jnp.where(rank < 2, 1, 6 - 2 * rank)
        return (my_plane + sign * away) * plane + lax.rem(me + c, plane)

    def fetch(c):
        source = pl.ds(pl.multiple_of(place(c) * rows, rows), rows)
        side = lax.rem(c, 2)
        return pltpu.make_async_copy(xs.at[:, source, :], x_buf.at[side], x_sems.at[side])

    fetch(0).start()
    squares[...] = jnp.zeros_like(squares)

    def remotes(c, owner):
        return (
            pltpu.make_async_remote_copy(
                src_ref=send_main.at[c], dst_ref=recv_main.at[:, my_rows, :],
                send_sem=main_sems.at[c], recv_sem=main_recv_sems.at[me],
                device_id={"wide": owner}, device_id_type=MESH,
            ),
            pltpu.make_async_remote_copy(
                src_ref=send_rest.at[c], dst_ref=recv_rest.at[my_rows, :],
                send_sem=rest_sems.at[c], recv_sem=rest_recv_sems.at[me],
                device_id={"wide": owner}, device_id_type=MESH,
            ),
        )

    def locals_(c):
        return (
            pltpu.make_async_copy(send_main.at[c], recv_main.at[:, my_rows, :], own_sems.at[0]),
            pltpu.make_async_copy(send_rest.at[c], recv_rest.at[my_rows, :], own_sems.at[1]),
        )

    def dispatch(c):
        owner = place(c)

        @pl.when(owner != me)
        def _():
            for copy in remotes(c, owner):
                copy.start()

        @pl.when(owner == me)
        def _():
            for copy in locals_(c):
                copy.start()

    lane = lax.broadcasted_iota(jnp.int32, (pair_rows, LANES), 1)

    def block(c, carry):
        @pl.when(c + 1 < n)
        def _():
            fetch(c + 1).start()

        fetch(c).wait()
        for k in range(deep):
            high, low = split(x_buf[lax.rem(c, 2), k])
            x_high[:, k * LANES : (k + 1) * LANES] = high
            x_low[:, k * LANES : (k + 1) * LANES] = low

        @pl.when(c == 1)
        def _():
            pl.semaphore_wait(barrier, n - 1)

        @pl.when(c > 0)
        def _():
            dispatch(c - 1)

        dot = functools.partial(jnp.dot, preferred_element_type=jnp.float32)
        small = dot(x_low[...], w_high[...]) + dot(x_high[...], w_low[...])
        product = (dot(x_high[...], w_high[...]) + small).reshape(span, pair_rows, -1) * scales[...][None]
        squares[...] = squares[...] + jnp.sum(product * product, axis=0)
        send_main[c] = product[:, :, :full]
        packed = [jnp.zeros((pair_rows, LANES), jnp.float32)] * (span * rest // LANES)
        for s in range(span):
            at, offset = divmod(s * rest, LANES)
            value = product[s, :, full:]
            if offset:
                value = pltpu.roll(value, offset, axis=1)
            if offset + rest > LANES:
                packed[at] = jnp.where(lane >= offset, value, packed[at])
                packed[at + 1] = jnp.where(lane < offset, value, packed[at + 1])
            else:
                packed[at] = jnp.where(lane >= offset, value, packed[at])
        for b, value in enumerate(packed):
            send_rest[c, :, b * LANES : (b + 1) * LANES] = value

        return carry

    lax.fori_loop(0, n, block, 0)
    dispatch(n - 1)
    total = squares[:, :LANES]
    for b in range(1, squares.shape[1] // LANES):
        total = total + squares[:, b * LANES : (b + 1) * LANES]
    sq_send[...] = total

    def sq_copy(src, dst, j):
        return pltpu.make_async_remote_copy(
            src_ref=sq_send, dst_ref=sq_recv.at[src],
            send_sem=sq_sems.at[j], recv_sem=sq_recv_sems.at[src],
            device_id={"wide": dst}, device_id_type=MESH,
        )

    for copy in remotes(0, place(0)):
        copy.wait_send()
    own_squares = pltpu.make_async_copy(sq_send, sq_recv.at[me], own_sems.at[2])
    own_squares.start()

    def send_squares(j, carry):
        sq_copy(me, lax.rem(me + j, n), j).start()
        return carry

    lax.fori_loop(1, n, send_squares, 0)
    own_squares.wait()

    def finish_sends(c, carry):
        owner = place(c)

        @pl.when(owner != me)
        def _():
            for copy in remotes(c, owner):
                copy.wait_send()

        @pl.when(owner == me)
        def _():
            for copy in locals_(c):
                copy.wait()

        return carry

    lax.fori_loop(1, n, finish_sends, 0)

    def finish(j, carry):
        src = lax.rem(me + j, n)
        rows = pl.ds(pl.multiple_of(src * pair_rows, pair_rows), pair_rows)
        pltpu.make_async_remote_copy(
            src_ref=send_main.at[0], dst_ref=recv_main.at[:, rows, :],
            send_sem=main_sems.at[0], recv_sem=main_recv_sems.at[src],
            device_id={"wide": src}, device_id_type=MESH,
        ).wait_recv()
        pltpu.make_async_remote_copy(
            src_ref=send_rest.at[0], dst_ref=recv_rest.at[rows, :],
            send_sem=rest_sems.at[0], recv_sem=rest_recv_sems.at[src],
            device_id={"wide": src}, device_id_type=MESH,
        ).wait_recv()
        sq_copy(src, src, j).wait_recv()
        sq_copy(me, src, j).wait_send()
        return carry

    lax.fori_loop(1, n, finish, 0)


def unpack_kernel(count, main_ref, rest_ref, sq_ref, out_ref, rms_ref, turned):
    group, pairs, full = main_ref.shape
    rest = out_ref.shape[1] - full
    step = pl.program_id(0)

    @pl.when(step == 0)
    def _():
        for b in range(rest_ref.shape[1] // LANES):
            turned[b * LANES : (b + 1) * LANES, :] = rest_ref[:, b * LANES : (b + 1) * LANES].T
        totals = jnp.sum(sq_ref[...].T, axis=0, keepdims=True)
        rms_ref[...] = jnp.sqrt(totals / count + 1e-06)

    for g in range(group):
        for b in range(full // LANES):
            out_ref[g, b * LANES : (b + 1) * LANES, :] = main_ref[g, :, b * LANES : (b + 1) * LANES].T
        start = pl.multiple_of((step * group + g) * rest, 8)
        out_ref[g, full:, :] = turned[pl.ds(start, rest), :]


def shards(n, half_integrals, pair_list, occupied_energy, virtual_orbitals, tile_order):
    pair_rows, columns, basis = half_integrals.shape
    virtuals = virtual_orbitals.shape[1]
    pairs = n * pair_rows
    span = columns // n
    deep = round_up(basis, LANES)
    broad = round_up(virtuals, LANES)
    full = virtuals // LANES * LANES
    rest = virtuals - full
    rows = span * pair_rows
    group = 4
    flops = 6 * pair_rows * columns * basis * virtuals
    vmem = pl.BlockSpec(memory_space=pltpu.VMEM)
    anywhere = pl.BlockSpec(memory_space=pl.ANY)

    def whole(*shape):
        return pl.BlockSpec(shape, lambda i: (0,) * len(shape))

    tiles = LANES // TILE_S
    xs, w_high, w_low, scales = pl.pallas_call(
        prepare_kernel,
        grid=(columns // LANES,),
        out_shape=(
            jax.ShapeDtypeStruct((deep // LANES, columns * pair_rows, LANES), jnp.float32),
            jax.ShapeDtypeStruct((deep, broad), jnp.bfloat16),
            jax.ShapeDtypeStruct((deep, broad), jnp.bfloat16),
            jax.ShapeDtypeStruct((pair_rows, broad), jnp.float32),
        ),
        in_specs=[
            pl.BlockSpec(memory_space=pltpu.SMEM),
            whole(2, pairs),
            whole(1, occupied_energy.shape[0]),
            pl.BlockSpec((pair_rows, basis, LANES), lambda i: (0, 0, i)),
            whole(basis, virtuals),
        ],
        out_specs=(anywhere, whole(deep, broad), whole(deep, broad), whole(pair_rows, broad)),
        scratch_shapes=[
            pltpu.VMEM((pairs, LANES), jnp.float32),
            pltpu.VMEM((2, deep // LANES, LANES * pair_rows, LANES), jnp.float32),
            pltpu.SMEM(tile_order.shape, jnp.int32),
            pltpu.SemaphoreType.DMA((2, tiles)),
        ],
        compiler_params=pltpu.CompilerParams(vmem_limit_bytes=28 * 1024 * 1024),
        name="prepare",
    )(tile_order, pair_list.T, occupied_energy.reshape(1, -1), pltpu.with_memory_space_constraint(jnp.swapaxes(half_integrals, 1, 2), pltpu.HBM), virtual_orbitals)
    recv_main, recv_rest, sq_recv = pl.pallas_call(
        functools.partial(exchange_kernel, n),
        out_shape=(
            jax.ShapeDtypeStruct((span, pairs, full), jnp.float32),
            jax.ShapeDtypeStruct((pairs, span * rest), jnp.float32),
            jax.ShapeDtypeStruct((n, pair_rows, LANES), jnp.float32),
        ),
        in_specs=[anywhere, vmem, vmem, vmem],
        out_specs=(anywhere, anywhere, anywhere),
        scratch_shapes=[
            pltpu.VMEM((2, deep // LANES, rows, LANES), jnp.float32),
            pltpu.VMEM((rows, deep), jnp.bfloat16),
            pltpu.VMEM((rows, deep), jnp.bfloat16),
            pltpu.VMEM((pair_rows, broad), jnp.float32),
            pltpu.VMEM((pair_rows, LANES), jnp.float32),
            pltpu.VMEM((n, span, pair_rows, full), jnp.float32),
            pltpu.VMEM((n, pair_rows, span * rest), jnp.float32),
            pltpu.SemaphoreType.DMA((2,)),
            pltpu.SemaphoreType.DMA((n,)),
            pltpu.SemaphoreType.DMA((n,)),
            pltpu.SemaphoreType.DMA((n,)),
            pltpu.SemaphoreType.DMA((n,)),
            pltpu.SemaphoreType.DMA((n,)),
            pltpu.SemaphoreType.DMA((n,)),
            pltpu.SemaphoreType.DMA((3,)),
        ],
        compiler_params=pltpu.CompilerParams(
            collective_id=0, has_side_effects=True, vmem_limit_bytes=20 * 1024 * 1024
        ),
        cost_estimate=pl.CostEstimate(flops=flops, bytes_accessed=4 * half_integrals.size, transcendentals=0),
        name="exchange",
    )(xs, w_high, w_low, scales)
    out, rms = pl.pallas_call(
        functools.partial(unpack_kernel, columns * virtuals),
        grid=(span // group,),
        out_shape=(
            jax.ShapeDtypeStruct((span, virtuals, pairs), jnp.float32),
            jax.ShapeDtypeStruct((1, pairs), jnp.float32),
        ),
        in_specs=[
            pl.BlockSpec((group, pairs, full), lambda i: (i, 0, 0)),
            pl.BlockSpec((pairs, span * rest), lambda i: (0, 0)),
            pl.BlockSpec((pairs, LANES), lambda i: (0, 0)),
        ],
        out_specs=(
            pl.BlockSpec((group, virtuals, pairs), lambda i: (i, 0, 0)),
            pl.BlockSpec((1, pairs), lambda i: (0, 0)),
        ),
        scratch_shapes=[pltpu.VMEM((span * rest, pairs), jnp.float32)],
        compiler_params=pltpu.CompilerParams(vmem_limit_bytes=20 * 1024 * 1024),
        name="unpack",
    )(recv_main, recv_rest, sq_recv.reshape(pairs, LANES))
    return (jnp.transpose(out, (2, 0, 1)), rms.reshape(-1))


def solution(mesh):
    in_specs = (
        P(("groups", "wide"), None, None),
        P("groups", None),
        P("groups"),
        P("groups", None),
        P(),
    )
    out_specs = (P("groups", "wide", None), P("groups"))
    return jax.shard_map(
        functools.partial(shards, mesh.shape["wide"]),
        mesh=mesh, in_specs=in_specs, out_specs=out_specs, check_vma=False,
    )
```

```python
import functools
import math

import jax
import jax.numpy as jnp
from jax import lax
from jax.experimental import pallas as pl
from jax.experimental.pallas import tpu as pltpu
from jax.sharding import PartitionSpec as P

TILE_S = 8
LANES = 128
EARLY = 2
MESH = pl.DeviceIdType.MESH


def round_up(value, step):
    return (value + step - 1) // step * step


def split(value):
    high = value.astype(jnp.bfloat16)
    low = (value - high.astype(jnp.float32)).astype(jnp.bfloat16)
    return high, low


def schedule(span, rest):
    wide = LANES // math.gcd(rest, LANES)
    sets = [("pair", p) for p in range(EARLY)]
    for g in range(span // wide):
        sets.append(("rest", g))
        sets += [("main", g * wide // TILE_S + k) for k in range(wide // TILE_S)]
    return wide, sets


def exchange_kernel(
    n, rest, order_hbm, pair_hbm, energy_hbm, x_hbm, w_hbm, out_ref, sq_recv,
    order_ref, pair_ref, energy_ref, index_buf, w_buf, x_buf, turned, x_high, x_low, w_high, w_low, scales, squares,
    send_main, rest_rows, send_rest, sq_send, recv_main, recv_rest, rest_turned,
    small_sems, w_sem, x_sems, send_sems, recv_sems, sq_sems, sq_recv_sems,
):
    me = lax.axis_index("wide")
    pair_rows, basis, columns = x_hbm.shape
    virtuals = w_hbm.shape[1]
    span, _, pairs = out_ref.shape
    full = virtuals - rest
    deep = turned.shape[1]
    groups = full // LANES
    plane = n // 4
    half = n // 2
    rows = half * span
    own = 3 * plane
    owner_tiles = span // TILE_S
    stride = recv_main.shape[2]
    wide, sets = schedule(span, rest)
    late = pair_rows - EARLY
    my_pair = pl.multiple_of(me * pair_rows, pair_rows)

    barrier = pltpu.get_barrier_semaphore()

    def greet(j, carry):
        pl.semaphore_signal(barrier, inc=1, device_id={"wide": lax.rem(me + j, n)}, device_id_type=MESH)
        return carry

    small = [
        pltpu.make_async_copy(order_hbm, order_ref, small_sems.at[0]),
        pltpu.make_async_copy(pair_hbm, pair_ref, small_sems.at[1]),
        pltpu.make_async_copy(energy_hbm, energy_ref, small_sems.at[2]),
    ]
    weights_copy = pltpu.make_async_copy(w_hbm, w_buf, w_sem.at[0])

    def fetch(p):
        return pltpu.make_async_copy(x_hbm.at[p], x_buf.at[p], x_sems.at[p])

    weights_copy.start()
    fetch(0).start()
    for copy in small:
        copy.start()
    for p in range(1, pair_rows):
        fetch(p).start()
    lax.fori_loop(1, n, greet, 0)

    sign = 1 - 2 * (me // half)
    my_plane = me // plane
    inner = jnp.minimum(my_plane, 3 - my_plane)

    def place(c):
        rank = c // plane
        away = 3 - rank - inner * jnp.where(rank < 2, 1, 6 - 2 * rank)
        return (my_plane + sign * away) * plane + lax.rem(me + c, plane)

    squares[...] = jnp.zeros_like(squares)
    w_high[...] = jnp.zeros_like(w_high)
    w_low[...] = jnp.zeros_like(w_low)
    for copy in small:
        copy.wait()
    orbitals = energy_ref.shape[1]
    orbital = lax.broadcasted_iota(jnp.int32, (pair_rows, orbitals), 1).astype(jnp.float32)
    energy = jnp.zeros((pair_rows, 1), jnp.float32)
    for k in range(2):
        line = pair_ref[k : k + 1, :].astype(jnp.float32)
        index_buf[...] = jnp.broadcast_to(line, (LANES, pairs)).T
        hit = index_buf[pl.ds(my_pair, pair_rows), 0:1] == orbital
        energy = energy + jnp.sum(jnp.where(hit, energy_ref[...], 0.0), axis=1, keepdims=True)
    scales[...] = jnp.broadcast_to(jnp.exp(0.3 * energy), scales.shape)
    weights_copy.wait()
    high, low = split(w_buf[...])
    w_high[:basis, :virtuals] = high
    w_low[:basis, :virtuals] = low

    def remote(i, c, owner):
        kind, at = sets[i]
        if kind == "pair":
            src = send_main.at[c, :, at, :, :]
            dst = recv_main.at[:, my_pair + at, pl.ds(0, span), :]
        elif kind == "main":
            src = send_main.at[c, :, pl.ds(EARLY, late), pl.ds(at * TILE_S, TILE_S), :]
            dst = recv_main.at[:, pl.ds(my_pair + EARLY, late), pl.ds(at * TILE_S, TILE_S), :]
        else:
            lanes = pl.ds(at * wide * rest, wide * rest)
            src = send_rest.at[c, :, lanes]
            dst = recv_rest.at[pl.ds(my_pair, pair_rows), lanes]
        return pltpu.make_async_remote_copy(
            src_ref=src, dst_ref=dst, send_sem=send_sems.at[i, c], recv_sem=recv_sems.at[i, me],
            device_id={"wide": owner}, device_id_type=MESH,
        )

    def arrival(i, src):
        kind, at = sets[i]
        first = pl.multiple_of(src * pair_rows, pair_rows)
        if kind == "pair":
            local = send_main.at[0, :, at, :, :]
            dst = recv_main.at[:, first + at, pl.ds(0, span), :]
        elif kind == "main":
            local = send_main.at[0, :, pl.ds(EARLY, late), pl.ds(at * TILE_S, TILE_S), :]
            dst = recv_main.at[:, pl.ds(first + EARLY, late), pl.ds(at * TILE_S, TILE_S), :]
        else:
            lanes = pl.ds(at * wide * rest, wide * rest)
            local = send_rest.at[0, :, lanes]
            dst = recv_rest.at[pl.ds(first, pair_rows), lanes]
        return pltpu.make_async_remote_copy(
            src_ref=local, dst_ref=dst, send_sem=send_sems.at[i, 0], recv_sem=recv_sems.at[i, src],
            device_id={"wide": src}, device_id_type=MESH,
        )

    def send(i, first, last):
        def one(c, carry):
            remote(i, c, place(c)).start()
            return carry

        lax.fori_loop(first, min(last, own), one, 0)
        lax.fori_loop(max(first, own + 1), last, one, 0)

    def compute(step, carry):
        p = step // 2
        part = lax.rem(step, 2)

        @pl.when(part == 0)
        def _():
            fetch(p).wait()
            for k in range(deep // LANES):
                size = min(LANES, basis - k * LANES)
                for b in range(columns // LANES):
                    piece = x_buf[p, k * LANES : k * LANES + size, b * LANES : (b + 1) * LANES]
                    if size < LANES:
                        piece = jnp.concatenate([piece, jnp.zeros((LANES - size, LANES), jnp.float32)], axis=0)
                    turned[b * LANES : (b + 1) * LANES, k * LANES : (k + 1) * LANES] = piece.T

        def gather(u, carry):
            pieces = []
            for v in range(2):
                at = u * 2 + v
                slot = place(part * half + at // owner_tiles) * owner_tiles + lax.rem(at, owner_tiles)
                pieces.append(turned[pl.ds(order_ref[slot] * TILE_S, TILE_S), :])
            high, low = split(jnp.concatenate(pieces, axis=0))
            block = pl.ds(pl.multiple_of(u * 2 * TILE_S, 2 * TILE_S), 2 * TILE_S)
            x_high[block, :] = high
            x_low[block, :] = low
            return carry

        lax.fori_loop(0, rows // TILE_S // 2, gather, 0, unroll=2)
        dot = functools.partial(jnp.dot, preferred_element_type=jnp.float32)
        small = dot(x_low[...], w_high[...]) + dot(x_high[...], w_low[...])
        product = dot(x_high[...], w_high[...]) + small
        scale = scales[pl.ds(p, 1), :]
        total = squares[p]
        first = part * half
        for b in range(product.shape[1] // LANES):
            value = product[:, b * LANES : (b + 1) * LANES] * scale
            total = total + jnp.sum((value * value).reshape(rows // TILE_S, TILE_S, LANES), axis=0)
            if b < groups:
                send_main[pl.ds(first, half), b, p, :, :] = value.reshape(half, span, LANES)
            else:
                rest_rows[pl.ds(first * span * pair_rows + p, rows, stride=pair_rows), :] = value
        squares[p] = total

        @pl.when(step == 0)
        def _():
            pl.semaphore_wait(barrier, n - 1)

        for early in range(EARLY):
            for h in range(2):
                @pl.when(step == early * 2 + h)
                def _():
                    send(early, h * half, (h + 1) * half)

        return carry

    lax.fori_loop(0, 2 * pair_rows, compute, 0)

    lane = lax.broadcasted_iota(jnp.int32, (pair_rows, LANES), 1)

    def pack(c, carry):
        packed = [jnp.zeros((pair_rows, LANES), jnp.float32)] * (span * rest // LANES)
        for s in range(span):
            at, offset = divmod(s * rest, LANES)
            value = rest_rows[pl.ds(pl.multiple_of((c * span + s) * pair_rows, pair_rows), pair_rows), :]
            if offset:
                value = pltpu.roll(value, offset, axis=1)
            if offset + rest > LANES:
                packed[at] = jnp.where(lane >= offset, value, packed[at])
                packed[at + 1] = jnp.where(lane < offset, value, packed[at + 1])
            else:
                packed[at] = jnp.where(lane >= offset, value, packed[at])
        for b, value in enumerate(packed):
            send_rest[c, :, b * LANES : (b + 1) * LANES] = value
        return carry

    lax.fori_loop(0, n, pack, 0)
    for p in range(pair_rows):
        sq_send[p : p + 1, :] = jnp.sum(squares[p], axis=0, keepdims=True)

    def sq_copy(src, dst, j):
        return pltpu.make_async_remote_copy(
            src_ref=sq_send, dst_ref=sq_recv.at[src],
            send_sem=sq_sems.at[j], recv_sem=sq_recv_sems.at[src],
            device_id={"wide": dst}, device_id_type=MESH,
        )

    def send_squares(j, carry):
        sq_copy(me, lax.rem(me + j, n), j).start()
        return carry

    for i in range(EARLY, len(sets)):
        send(i, 0, n)
        if i == EARLY:
            lax.fori_loop(1, n, send_squares, 0)
    sq_recv[me] = sq_send[...]
    recv_main[:, pl.ds(my_pair, pair_rows), :span, :] = send_main[own]
    recv_rest[pl.ds(my_pair, pair_rows), :] = send_rest[own]

    lines = recv_main.reshape(groups * pairs * stride, LANES)

    def wait_set(i):
        def one(j, carry):
            arrival(i, lax.rem(me + j, n)).wait_recv()
            return carry

        lax.fori_loop(1, n, one, 0)

    for i, (kind, at) in enumerate(sets):
        wait_set(i)
        if kind == "rest":
            for b in range(at * wide * rest // LANES, (at + 1) * wide * rest // LANES):
                for q in range(pairs // LANES):
                    rest_turned[b * LANES : (b + 1) * LANES, q * LANES : (q + 1) * LANES] = (
                        recv_rest[q * LANES : (q + 1) * LANES, b * LANES : (b + 1) * LANES].T
                    )
        elif kind == "main":
            def assemble(k, carry):
                s = at * TILE_S + k
                for b in range(groups):
                    for q in range(pairs // LANES):
                        first = (b * pairs + q * LANES) * stride + s
                        out_ref[s, b * LANES : (b + 1) * LANES, q * LANES : (q + 1) * LANES] = (
                            lines[pl.ds(first, LANES, stride=stride), :].T
                        )
                out_ref[s, full:, :] = rest_turned[pl.ds(pl.multiple_of(s * rest, 8), rest), :]
                return carry

            lax.fori_loop(0, TILE_S, assemble, 0)

    def finish(j, carry):
        src = lax.rem(me + j, n)
        sq_copy(src, src, j).wait_recv()
        sq_copy(me, src, j).wait_send()
        return carry

    lax.fori_loop(1, n, finish, 0)
    for i in range(len(sets)):
        def sent(c, carry):
            remote(i, c, place(c)).wait_send()
            return carry

        lax.fori_loop(0, own, sent, 0)
        lax.fori_loop(own + 1, n, sent, 0)


def finish_kernel(count, main_ref, sq_ref, out_ref, rms_ref, sems):
    parts = sems.shape[0]
    size = main_ref.shape[0] // parts
    copies = [
        pltpu.make_async_copy(main_ref.at[pl.ds(i * size, size)], out_ref.at[pl.ds(i * size, size)], sems.at[i])
        for i in range(parts)
    ]
    for copy in copies:
        copy.start()
    totals = jnp.sum(sq_ref[...].T, axis=0, keepdims=True)
    rms_ref[...] = jnp.sqrt(totals / count + 1e-06)
    for copy in copies:
        copy.wait()


def shards(n, half_integrals, pair_list, occupied_energy, virtual_orbitals, tile_order):
    pair_rows, columns, basis = half_integrals.shape
    virtuals = virtual_orbitals.shape[1]
    pairs = n * pair_rows
    span = columns // n
    deep = round_up(basis, LANES)
    broad = round_up(virtuals, LANES)
    full = virtuals // LANES * LANES
    rest = virtuals - full
    groups = full // LANES
    count = len(schedule(span, rest)[1])
    flops = 6 * pair_rows * columns * basis * virtuals
    vmem = pl.BlockSpec(memory_space=pltpu.VMEM)
    anywhere = pl.BlockSpec(memory_space=pl.ANY)

    def hbm(value):
        return pltpu.with_memory_space_constraint(value, pltpu.HBM)

    main, sq_recv = pl.pallas_call(
        functools.partial(exchange_kernel, n, rest),
        out_shape=(
            pltpu.VMEM((span, virtuals, pairs), jnp.float32),
            pltpu.VMEM((n, pair_rows, LANES), jnp.float32),
        ),
        in_specs=[anywhere] * 5,
        out_specs=(vmem, vmem),
        scratch_shapes=[
            pltpu.SMEM(tile_order.shape, jnp.int32),
            pltpu.VMEM((2, pairs), jnp.int32),
            pltpu.VMEM((1, occupied_energy.shape[0]), jnp.float32),
            pltpu.VMEM((pairs, LANES), jnp.float32),
            pltpu.VMEM((basis, virtuals), jnp.float32),
            pltpu.VMEM((pair_rows, basis, columns), jnp.float32),
            pltpu.VMEM((columns, deep), jnp.float32),
            pltpu.VMEM((columns // 2, deep), jnp.bfloat16),
            pltpu.VMEM((columns // 2, deep), jnp.bfloat16),
            pltpu.VMEM((deep, broad), jnp.bfloat16),
            pltpu.VMEM((deep, broad), jnp.bfloat16),
            pltpu.VMEM((pair_rows, LANES), jnp.float32),
            pltpu.VMEM((pair_rows, TILE_S, LANES), jnp.float32),
            pltpu.VMEM((n, groups, pair_rows, span, LANES), jnp.float32),
            pltpu.VMEM((columns * pair_rows, LANES), jnp.float32),
            pltpu.VMEM((n, pair_rows, span * rest), jnp.float32),
            pltpu.VMEM((pair_rows, LANES), jnp.float32),
            pltpu.VMEM((groups, pairs, span + TILE_S, LANES), jnp.float32),
            pltpu.VMEM((pairs, span * rest), jnp.float32),
            pltpu.VMEM((span * rest, pairs), jnp.float32),
            pltpu.SemaphoreType.DMA((3,)),
            pltpu.SemaphoreType.DMA((1,)),
            pltpu.SemaphoreType.DMA((pair_rows,)),
            pltpu.SemaphoreType.DMA((count, n)),
            pltpu.SemaphoreType.DMA((count, n)),
            pltpu.SemaphoreType.DMA((n,)),
            pltpu.SemaphoreType.DMA((n,)),
        ],
        compiler_params=pltpu.CompilerParams(
            collective_id=0, has_side_effects=True, vmem_limit_bytes=52 * 1024 * 1024
        ),
        cost_estimate=pl.CostEstimate(flops=flops, bytes_accessed=4 * half_integrals.size, transcendentals=0),
        name="exchange",
    )(
        hbm(tile_order), hbm(pair_list.T), hbm(occupied_energy.reshape(1, -1)),
        hbm(jnp.swapaxes(half_integrals, 1, 2)), hbm(virtual_orbitals),
    )
    out, rms = pl.pallas_call(
        functools.partial(finish_kernel, columns * virtuals),
        out_shape=(
            jax.ShapeDtypeStruct((span, virtuals, pairs), jnp.float32),
            jax.ShapeDtypeStruct((1, pairs), jnp.float32),
        ),
        in_specs=[vmem, vmem],
        out_specs=(pl.BlockSpec(memory_space=pltpu.HBM), vmem),
        scratch_shapes=[pltpu.SemaphoreType.DMA((8,))],
        compiler_params=pltpu.CompilerParams(vmem_limit_bytes=2 * 1024 * 1024),
        name="finish",
    )(main, sq_recv.reshape(pairs, LANES))
    return (jnp.transpose(out, (2, 0, 1)), rms.reshape(-1))


def solution(mesh):
    in_specs = (
        P(("groups", "wide"), None, None),
        P("groups", None),
        P("groups"),
        P("groups", None),
        P(),
    )
    out_specs = (P("groups", "wide", None), P("groups"))
    return jax.shard_map(
        functools.partial(shards, mesh.shape["wide"]),
        mesh=mesh, in_specs=in_specs, out_specs=out_specs, check_vma=False,
    )
```

```python
import functools
import math

import jax
import jax.numpy as jnp
from jax import lax
from jax.experimental import pallas as pl
from jax.experimental.pallas import tpu as pltpu
from jax.sharding import PartitionSpec as P

TILE_S = 8
LANES = 128
EARLY = 2
PARTS = 4
AHEAD = 2
MESH = pl.DeviceIdType.MESH


def round_up(value, step):
    return (value + step - 1) // step * step


def split(value):
    high = value.astype(jnp.bfloat16)
    low = (value - high.astype(jnp.float32)).astype(jnp.bfloat16)
    return high, low


def schedule(span, rest):
    wide = LANES // math.gcd(rest, LANES)
    sets = [("pair", p) for p in range(EARLY)]
    for g in range(span // wide):
        sets.append(("rest", g))
        sets += [("main", g * wide // TILE_S + k) for k in range(wide // TILE_S)]
    return wide, sets


def exchange_kernel(
    n, rest, order_hbm, pair_hbm, energy_hbm, x_hbm, w_hbm, out_ref, recv_main, rest_turned, sq_recv,
    order_ref, pair_ref, energy_ref, index_buf, w_buf, x_buf, turned, x_high, x_low, w_high, w_low, scales, squares,
    send_main, rest_rows, send_rest, sq_send, recv_rest,
    small_sems, w_sem, x_sems, send_sems, recv_sems, sq_sems, sq_recv_sems,
):
    me = lax.axis_index("wide")
    pair_rows, basis, columns = x_hbm.shape
    virtuals = w_hbm.shape[1]
    pairs = recv_main.shape[1]
    span = columns // n
    full = virtuals - rest
    deep = turned.shape[1]
    groups = full // LANES
    plane = n // 4
    half = n // 2
    owners = n // PARTS
    rows = owners * span
    own = 3 * plane
    owner_tiles = span // TILE_S
    stride = recv_main.shape[2]
    wide, sets = schedule(span, rest)
    late = pair_rows - EARLY
    my_pair = pl.multiple_of(me * pair_rows, pair_rows)

    barrier = pltpu.get_barrier_semaphore()

    def greet(j, carry):
        pl.semaphore_signal(barrier, inc=1, device_id={"wide": lax.rem(me + j, n)}, device_id_type=MESH)
        return carry

    small = [
        pltpu.make_async_copy(order_hbm, order_ref, small_sems.at[0]),
        pltpu.make_async_copy(pair_hbm, pair_ref, small_sems.at[1]),
        pltpu.make_async_copy(energy_hbm, energy_ref, small_sems.at[2]),
    ]
    weights_copy = pltpu.make_async_copy(w_hbm, w_buf, w_sem.at[0])

    def fetch(p):
        return pltpu.make_async_copy(x_hbm.at[p], x_buf.at[p], x_sems.at[p])

    fetch(0).start()
    weights_copy.start()
    for copy in small:
        copy.start()
    lax.fori_loop(1, n, greet, 0)

    sign = 1 - 2 * (me // half)
    my_plane = me // plane
    inner = jnp.minimum(my_plane, 3 - my_plane)

    def place(c):
        rank = c // plane
        away = 3 - rank - inner * jnp.where(rank < 2, 1, 6 - 2 * rank)
        return (my_plane + sign * away) * plane + lax.rem(me + c, plane)

    squares[...] = jnp.zeros_like(squares)
    w_high[...] = jnp.zeros_like(w_high)
    w_low[...] = jnp.zeros_like(w_low)
    for copy in small:
        copy.wait()
    orbitals = energy_ref.shape[1]
    orbital = lax.broadcasted_iota(jnp.int32, (pair_rows, orbitals), 1).astype(jnp.float32)
    energy = jnp.zeros((pair_rows, 1), jnp.float32)
    for k in range(2):
        line = pair_ref[k : k + 1, :].astype(jnp.float32)
        index_buf[...] = jnp.broadcast_to(line, (LANES, pairs)).T
        hit = index_buf[pl.ds(my_pair, pair_rows), 0:1] == orbital
        energy = energy + jnp.sum(jnp.where(hit, energy_ref[...], 0.0), axis=1, keepdims=True)
    scales[...] = jnp.broadcast_to(jnp.exp(0.3 * energy), scales.shape)
    weights_copy.wait()
    for p in range(1, AHEAD):
        fetch(p).start()
    high, low = split(w_buf[...])
    w_high[:basis, :virtuals] = high
    w_low[:basis, :virtuals] = low

    def remote(i, c, owner):
        kind, at = sets[i]
        if kind == "pair":
            src = send_main.at[c, :, at, :, :]
            dst = recv_main.at[:, my_pair + at, pl.ds(0, span), :]
        elif kind == "main":
            src = send_main.at[c, :, pl.ds(EARLY, late), pl.ds(at * TILE_S, TILE_S), :]
            dst = recv_main.at[:, pl.ds(my_pair + EARLY, late), pl.ds(at * TILE_S, TILE_S), :]
        else:
            lanes = pl.ds(at * wide * rest, wide * rest)
            src = send_rest.at[c, :, lanes]
            dst = recv_rest.at[pl.ds(my_pair, pair_rows), lanes]
        return pltpu.make_async_remote_copy(
            src_ref=src, dst_ref=dst, send_sem=send_sems.at[i, c], recv_sem=recv_sems.at[i, me],
            device_id={"wide": owner}, device_id_type=MESH,
        )

    def arrival(i, src):
        kind, at = sets[i]
        first = pl.multiple_of(src * pair_rows, pair_rows)
        if kind == "pair":
            local = send_main.at[0, :, at, :, :]
            dst = recv_main.at[:, first + at, pl.ds(0, span), :]
        elif kind == "main":
            local = send_main.at[0, :, pl.ds(EARLY, late), pl.ds(at * TILE_S, TILE_S), :]
            dst = recv_main.at[:, pl.ds(first + EARLY, late), pl.ds(at * TILE_S, TILE_S), :]
        else:
            lanes = pl.ds(at * wide * rest, wide * rest)
            local = send_rest.at[0, :, lanes]
            dst = recv_rest.at[pl.ds(first, pair_rows), lanes]
        return pltpu.make_async_remote_copy(
            src_ref=local, dst_ref=dst, send_sem=send_sems.at[i, 0], recv_sem=recv_sems.at[i, src],
            device_id={"wide": src}, device_id_type=MESH,
        )

    def send(i, first, last):
        def one(c, carry):
            remote(i, c, place(c)).start()
            return carry

        lax.fori_loop(first, min(last, own), one, 0)
        lax.fori_loop(max(first, own + 1), last, one, 0)

    def compute(step, carry):
        p = step // PARTS
        part = lax.rem(step, PARTS)

        @pl.when(part == 0)
        def _():
            fetch(p).wait()

            @pl.when(p + AHEAD < pair_rows)
            def _():
                fetch(p + AHEAD).start()

            for k in range(deep // LANES):
                size = min(LANES, basis - k * LANES)
                for b in range(columns // LANES):
                    piece = x_buf[p, k * LANES : k * LANES + size, b * LANES : (b + 1) * LANES]
                    if size < LANES:
                        piece = jnp.concatenate([piece, jnp.zeros((LANES - size, LANES), jnp.float32)], axis=0)
                    turned[b * LANES : (b + 1) * LANES, k * LANES : (k + 1) * LANES] = piece.T

        def gather(u, carry):
            pieces = []
            for v in range(2):
                at = u * 2 + v
                slot = place(part * owners + at // owner_tiles) * owner_tiles + lax.rem(at, owner_tiles)
                pieces.append(turned[pl.ds(order_ref[slot] * TILE_S, TILE_S), :])
            high, low = split(jnp.concatenate(pieces, axis=0))
            block = pl.ds(pl.multiple_of(u * 2 * TILE_S, 2 * TILE_S), 2 * TILE_S)
            x_high[block, :] = high
            x_low[block, :] = low
            return carry

        lax.fori_loop(0, rows // TILE_S // 2, gather, 0, unroll=8)
        dot = functools.partial(jnp.dot, preferred_element_type=jnp.float32)
        small = dot(x_low[...], w_high[...]) + dot(x_high[...], w_low[...])
        product = dot(x_high[...], w_high[...]) + small
        scale = scales[pl.ds(p, 1), :]
        total = squares[p]
        first = part * owners
        for b in range(product.shape[1] // LANES):
            value = product[:, b * LANES : (b + 1) * LANES] * scale
            total = total + jnp.sum((value * value).reshape(rows // TILE_S, TILE_S, LANES), axis=0)
            if b < groups:
                send_main[pl.ds(first, owners), b, p, :, :] = value.reshape(owners, span, LANES)
            else:
                rest_rows[pl.ds(first * span * pair_rows + p, rows, stride=pair_rows), :] = value
        squares[p] = total

        @pl.when(step == 0)
        def _():
            pl.semaphore_wait(barrier, n - 1)

        for early in range(EARLY):
            for h in range(PARTS):
                @pl.when(step == early * PARTS + h)
                def _():
                    send(early, h * owners, (h + 1) * owners)

        return carry

    lax.fori_loop(0, PARTS * pair_rows, compute, 0)

    lane = lax.broadcasted_iota(jnp.int32, (pair_rows, LANES), 1)

    def pack(c, carry):
        packed = [jnp.zeros((pair_rows, LANES), jnp.float32)] * (span * rest // LANES)
        for s in range(span):
            at, offset = divmod(s * rest, LANES)
            value = rest_rows[pl.ds(pl.multiple_of((c * span + s) * pair_rows, pair_rows), pair_rows), :]
            if offset:
                value = pltpu.roll(value, offset, axis=1)
            if offset + rest > LANES:
                packed[at] = jnp.where(lane >= offset, value, packed[at])
                packed[at + 1] = jnp.where(lane < offset, value, packed[at + 1])
            else:
                packed[at] = jnp.where(lane >= offset, value, packed[at])
        for b, value in enumerate(packed):
            send_rest[c, :, b * LANES : (b + 1) * LANES] = value
        return carry

    lax.fori_loop(0, n, pack, 0)
    for p in range(pair_rows):
        sq_send[p : p + 1, :] = jnp.sum(squares[p], axis=0, keepdims=True)

    def sq_copy(src, dst, j):
        return pltpu.make_async_remote_copy(
            src_ref=sq_send, dst_ref=sq_recv.at[src],
            send_sem=sq_sems.at[j], recv_sem=sq_recv_sems.at[src],
            device_id={"wide": dst}, device_id_type=MESH,
        )

    def send_squares(j, carry):
        sq_copy(me, lax.rem(me + j, n), j).start()
        return carry

    for i in range(EARLY, len(sets)):
        send(i, 0, n)
        if i == EARLY:
            lax.fori_loop(1, n, send_squares, 0)
    sq_recv[me] = sq_send[...]
    recv_main[:, pl.ds(my_pair, pair_rows), :span, :] = send_main[own]
    recv_rest[pl.ds(my_pair, pair_rows), :] = send_rest[own]

    def wait_set(i):
        def one(j, carry):
            arrival(i, lax.rem(me + j, n)).wait_recv()
            return carry

        lax.fori_loop(1, n, one, 0)

    def sent_set(i):
        def one(c, carry):
            remote(i, c, place(c)).wait_send()
            return carry

        lax.fori_loop(0, own, one, 0)
        lax.fori_loop(own + 1, n, one, 0)

    def finish(j, carry):
        src = lax.rem(me + j, n)
        sq_copy(src, src, j).wait_recv()
        sq_copy(me, src, j).wait_send()
        return carry

    last = len(sets) - 1
    for i, (kind, at) in enumerate(sets):
        if i == last:
            lax.fori_loop(1, n, finish, 0)
            for k in range(last):
                sent_set(k)
        wait_set(i)
        if kind == "rest":
            for b in range(at * wide * rest // LANES, (at + 1) * wide * rest // LANES):
                for q in range(pairs // LANES):
                    rest_turned[b * LANES : (b + 1) * LANES, q * LANES : (q + 1) * LANES] = (
                        recv_rest[q * LANES : (q + 1) * LANES, b * LANES : (b + 1) * LANES].T
                    )
        elif kind == "main" and i < last:
            def row(k, carry):
                assemble(recv_main, rest_turned, out_ref, at * TILE_S + k, at * TILE_S + k)
                return carry

            lax.fori_loop(0, TILE_S, row, 0)
    sent_set(last)


def assemble(recv_main, rest_turned, out_ref, s, to):
    groups, pairs, stride, _ = recv_main.shape
    full = groups * LANES
    rest = out_ref.shape[1] - full
    lines = recv_main.reshape(groups * pairs * stride, LANES)
    for b in range(groups):
        for q in range(pairs // LANES):
            first = (b * pairs + q * LANES) * stride + s
            out_ref[to, b * LANES : (b + 1) * LANES, q * LANES : (q + 1) * LANES] = (
                lines[pl.ds(first, LANES, stride=stride), :].T
            )
    out_ref[to, full:, :] = rest_turned[pl.ds(pl.multiple_of(s * rest, 8), rest), :]


def finish_kernel(count, main_ref, recv_main, rest_turned, sq_ref, out_ref, rms_ref, tail, rms, sems, tail_sems):
    done = main_ref.shape[0]
    copies = [
        pltpu.make_async_copy(main_ref.at[pl.ds(k, TILE_S)], out_ref.at[pl.ds(k, TILE_S)], sems.at[k // TILE_S])
        for k in range(0, done, TILE_S)
    ]
    for copy in copies:
        copy.start()
    totals = jnp.sum(sq_ref[...].T, axis=0, keepdims=True)
    rms[...] = jnp.sqrt(totals / count + 1e-06)
    rms_copy = pltpu.make_async_copy(rms, rms_ref, tail_sems.at[tail.shape[0]])
    rms_copy.start()
    copies.append(rms_copy)
    for k in range(tail.shape[0]):
        assemble(recv_main, rest_turned, tail, done + k, k)
        copy = pltpu.make_async_copy(tail.at[k], out_ref.at[done + k], tail_sems.at[k])
        copy.start()
        copies.append(copy)
    for copy in copies:
        copy.wait()


def shards(n, half_integrals, pair_list, occupied_energy, virtual_orbitals, tile_order):
    pair_rows, columns, basis = half_integrals.shape
    virtuals = virtual_orbitals.shape[1]
    pairs = n * pair_rows
    span = columns // n
    deep = round_up(basis, LANES)
    broad = round_up(virtuals, LANES)
    full = virtuals // LANES * LANES
    rest = virtuals - full
    groups = full // LANES
    count = len(schedule(span, rest)[1])
    flops = 6 * pair_rows * columns * basis * virtuals
    vmem = pl.BlockSpec(memory_space=pltpu.VMEM)
    anywhere = pl.BlockSpec(memory_space=pl.ANY)

    def hbm(value):
        return pltpu.with_memory_space_constraint(value, pltpu.HBM)

    main, recv_main, rest_turned, sq_recv = pl.pallas_call(
        functools.partial(exchange_kernel, n, rest),
        out_shape=(
            pltpu.VMEM((span - TILE_S, virtuals, pairs), jnp.float32),
            pltpu.VMEM((groups, pairs, span + TILE_S, LANES), jnp.float32),
            pltpu.VMEM((span * rest, pairs), jnp.float32),
            pltpu.VMEM((n, pair_rows, LANES), jnp.float32),
        ),
        in_specs=[anywhere] * 5,
        out_specs=(vmem,) * 4,
        scratch_shapes=[
            pltpu.SMEM(tile_order.shape, jnp.int32),
            pltpu.VMEM((2, pairs), jnp.int32),
            pltpu.VMEM((1, occupied_energy.shape[0]), jnp.float32),
            pltpu.VMEM((pairs, LANES), jnp.float32),
            pltpu.VMEM((basis, virtuals), jnp.float32),
            pltpu.VMEM((pair_rows, basis, columns), jnp.float32),
            pltpu.VMEM((columns, deep), jnp.float32),
            pltpu.VMEM((columns // PARTS, deep), jnp.bfloat16),
            pltpu.VMEM((columns // PARTS, deep), jnp.bfloat16),
            pltpu.VMEM((deep, broad), jnp.bfloat16),
            pltpu.VMEM((deep, broad), jnp.bfloat16),
            pltpu.VMEM((pair_rows, LANES), jnp.float32),
            pltpu.VMEM((pair_rows, TILE_S, LANES), jnp.float32),
            pltpu.VMEM((n, groups, pair_rows, span, LANES), jnp.float32),
            pltpu.VMEM((columns * pair_rows, LANES), jnp.float32),
            pltpu.VMEM((n, pair_rows, span * rest), jnp.float32),
            pltpu.VMEM((pair_rows, LANES), jnp.float32),
            pltpu.VMEM((pairs, span * rest), jnp.float32),
            pltpu.SemaphoreType.DMA((3,)),
            pltpu.SemaphoreType.DMA((1,)),
            pltpu.SemaphoreType.DMA((pair_rows,)),
            pltpu.SemaphoreType.DMA((count, n)),
            pltpu.SemaphoreType.DMA((count, n)),
            pltpu.SemaphoreType.DMA((n,)),
            pltpu.SemaphoreType.DMA((n,)),
        ],
        compiler_params=pltpu.CompilerParams(
            collective_id=0, has_side_effects=True, vmem_limit_bytes=42 * 1024 * 1024
        ),
        cost_estimate=pl.CostEstimate(flops=flops, bytes_accessed=4 * half_integrals.size, transcendentals=0),
        name="exchange",
    )(
        hbm(tile_order), hbm(pair_list.T), hbm(occupied_energy.reshape(1, -1)),
        hbm(jnp.swapaxes(half_integrals, 1, 2)), hbm(virtual_orbitals),
    )
    out, rms = pl.pallas_call(
        functools.partial(finish_kernel, columns * virtuals),
        out_shape=(
            jax.ShapeDtypeStruct((span, virtuals, pairs), jnp.float32),
            jax.ShapeDtypeStruct((1, pairs), jnp.float32),
        ),
        in_specs=[vmem] * 4,
        out_specs=(pl.BlockSpec(memory_space=pltpu.HBM),) * 2,
        scratch_shapes=[
            pltpu.VMEM((TILE_S, virtuals, pairs), jnp.float32),
            pltpu.VMEM((1, pairs), jnp.float32),
            pltpu.SemaphoreType.DMA((span // TILE_S - 1,)),
            pltpu.SemaphoreType.DMA((TILE_S + 1,)),
        ],
        compiler_params=pltpu.CompilerParams(vmem_limit_bytes=8 * 1024 * 1024),
        name="finish",
    )(main, recv_main, rest_turned, sq_recv.reshape(pairs, LANES))
    return (jnp.transpose(out, (2, 0, 1)), rms.reshape(-1))


def solution(mesh):
    in_specs = (
        P(("groups", "wide"), None, None),
        P("groups", None),
        P("groups"),
        P("groups", None),
        P(),
    )
    out_specs = (P("groups", "wide", None), P("groups"))
    return jax.shard_map(
        functools.partial(shards, mesh.shape["wide"]),
        mesh=mesh, in_specs=in_specs, out_specs=out_specs, check_vma=False,
    )
```

```python
import functools
import math

import jax
import jax.numpy as jnp
from jax import lax
from jax.experimental import pallas as pl
from jax.experimental.pallas import tpu as pltpu
from jax.sharding import PartitionSpec as P

TILE_S = 8
LANES = 128
EARLY = 2
PARTS = 4
AHEAD = 2
MESH = pl.DeviceIdType.MESH


def round_up(value, step):
    return (value + step - 1) // step * step


def split(value):
    high = value.astype(jnp.bfloat16)
    low = (value - high.astype(jnp.float32)).astype(jnp.bfloat16)
    return high, low


def schedule(span, rest):
    wide = LANES // math.gcd(rest, LANES)
    sets = [("pair", p) for p in range(EARLY)]
    for g in range(span // wide):
        sets.append(("rest", g))
        sets += [("main", g * wide // TILE_S + k) for k in range(wide // TILE_S)]
    return wide, sets


def exchange_kernel(
    n, rest, order_hbm, pair_hbm, energy_hbm, x_hbm, w_hbm, out_ref, recv_main, rest_turned, sq_recv,
    order_ref, pair_ref, energy_ref, index_buf, w_buf, x_buf, turned, x_high, x_low, w_high, w_low, scales, squares,
    send_main, rest_rows, send_rest, sq_send, recv_rest,
    small_sems, w_sem, x_sems, send_sems, recv_sems, sq_sems,
):
    me = lax.axis_index("wide")
    pair_rows, basis, columns = x_hbm.shape
    virtuals = w_hbm.shape[1]
    pairs = recv_main.shape[1]
    span = columns // n
    full = virtuals - rest
    deep = turned.shape[1]
    groups = full // LANES
    plane = n // 4
    half = n // 2
    owners = n // PARTS
    rows = owners * span
    own = 3 * plane
    owner_tiles = span // TILE_S
    stride = recv_main.shape[2]
    wide, sets = schedule(span, rest)
    late = pair_rows - EARLY
    my_pair = pl.multiple_of(me * pair_rows, pair_rows)

    barrier = pltpu.get_barrier_semaphore()

    def greet(j, carry):
        pl.semaphore_signal(barrier, inc=1, device_id={"wide": lax.rem(me + j, n)}, device_id_type=MESH)
        return carry

    small = [
        pltpu.make_async_copy(order_hbm, order_ref, small_sems.at[0]),
        pltpu.make_async_copy(pair_hbm, pair_ref, small_sems.at[1]),
        pltpu.make_async_copy(energy_hbm, energy_ref, small_sems.at[2]),
    ]
    weights_copy = pltpu.make_async_copy(w_hbm, w_buf, w_sem.at[0])

    def fetch(p):
        return pltpu.make_async_copy(x_hbm.at[p], x_buf.at[p], x_sems.at[lax.rem(p, AHEAD)])

    fetch(0).start()
    weights_copy.start()
    for copy in small:
        copy.start()
    lax.fori_loop(1, n, greet, 0)

    sign = 1 - 2 * (me // half)
    my_plane = me // plane
    inner = jnp.minimum(my_plane, 3 - my_plane)

    def place(c):
        rank = c // plane
        away = 3 - rank - inner * jnp.where(rank < 2, 1, 6 - 2 * rank)
        return (my_plane + sign * away) * plane + lax.rem(me + c, plane)

    squares[...] = jnp.zeros_like(squares)
    w_high[...] = jnp.zeros_like(w_high)
    w_low[...] = jnp.zeros_like(w_low)
    for copy in small:
        copy.wait()
    orbitals = energy_ref.shape[1]
    orbital = lax.broadcasted_iota(jnp.int32, (pair_rows, orbitals), 1).astype(jnp.float32)
    energy = jnp.zeros((pair_rows, 1), jnp.float32)
    for k in range(2):
        line = pair_ref[k : k + 1, :].astype(jnp.float32)
        index_buf[...] = jnp.broadcast_to(line, (LANES, pairs)).T
        hit = index_buf[pl.ds(my_pair, pair_rows), 0:1] == orbital
        energy = energy + jnp.sum(jnp.where(hit, energy_ref[...], 0.0), axis=1, keepdims=True)
    scales[...] = jnp.broadcast_to(jnp.exp(0.3 * energy), scales.shape)
    weights_copy.wait()
    for p in range(1, AHEAD):
        fetch(p).start()
    high, low = split(w_buf[...])
    w_high[:basis, :virtuals] = high
    w_low[:basis, :virtuals] = low

    def remote(i, c, owner):
        kind, at = sets[i]
        if kind == "pair":
            src = send_main.at[c, :, at, :, :]
            dst = recv_main.at[:, my_pair + at, pl.ds(0, span), :]
        elif kind == "main":
            src = send_main.at[c, :, pl.ds(EARLY, late), pl.ds(at * TILE_S, TILE_S), :]
            dst = recv_main.at[:, pl.ds(my_pair + EARLY, late), pl.ds(at * TILE_S, TILE_S), :]
        else:
            lanes = pl.ds(at * wide * rest, wide * rest)
            src = send_rest.at[c, :, lanes]
            dst = recv_rest.at[pl.ds(my_pair, pair_rows), lanes]
        return pltpu.make_async_remote_copy(
            src_ref=src, dst_ref=dst, send_sem=send_sems.at[i], recv_sem=recv_sems.at[i],
            device_id={"wide": owner}, device_id_type=MESH,
        )

    def wait_all(i, received):
        kind, at = sets[i]
        if kind == "pair":
            src = send_main.at[pl.ds(0, n - 1), :, at, :, :]
            dst = recv_main.at[:, pl.ds(0, n - 1), pl.ds(0, span), :]
        elif kind == "main":
            src = send_main.at[pl.ds(0, n - 1), :, pl.ds(EARLY, late), pl.ds(at * TILE_S, TILE_S), :]
            dst = recv_main.at[:, pl.ds(0, late * (n - 1)), pl.ds(at * TILE_S, TILE_S), :]
        else:
            lanes = pl.ds(at * wide * rest, wide * rest)
            src = send_rest.at[pl.ds(0, n - 1), :, lanes]
            dst = recv_rest.at[pl.ds(0, pair_rows * (n - 1)), lanes]
        ref, sem = (dst, recv_sems.at[i]) if received else (src, send_sems.at[i])
        pltpu.make_async_copy(ref, ref, sem).wait()

    def send(i, first, last):
        def one(c, carry):
            remote(i, c, place(c)).start()
            return carry

        lax.fori_loop(first, min(last, own), one, 0)
        lax.fori_loop(max(first, own + 1), last, one, 0)

    def compute(step, carry):
        p = step // PARTS
        part = lax.rem(step, PARTS)

        @pl.when(part == 0)
        def _():
            fetch(p).wait()

            @pl.when(p + AHEAD < pair_rows)
            def _():
                fetch(p + AHEAD).start()

            for k in range(deep // LANES):
                size = min(LANES, basis - k * LANES)
                for b in range(columns // LANES):
                    piece = x_buf[p, k * LANES : k * LANES + size, b * LANES : (b + 1) * LANES]
                    if size < LANES:
                        piece = jnp.concatenate([piece, jnp.zeros((LANES - size, LANES), jnp.float32)], axis=0)
                    turned[b * LANES : (b + 1) * LANES, k * LANES : (k + 1) * LANES] = piece.T

        def gather(u, carry):
            pieces = []
            for v in range(2):
                at = u * 2 + v
                slot = place(part * owners + at // owner_tiles) * owner_tiles + lax.rem(at, owner_tiles)
                pieces.append(turned[pl.ds(order_ref[slot] * TILE_S, TILE_S), :])
            high, low = split(jnp.concatenate(pieces, axis=0))
            block = pl.ds(pl.multiple_of(u * 2 * TILE_S, 2 * TILE_S), 2 * TILE_S)
            x_high[block, :] = high
            x_low[block, :] = low
            return carry

        lax.fori_loop(0, rows // TILE_S // 2, gather, 0, unroll=8)
        dot = functools.partial(jnp.dot, preferred_element_type=jnp.float32)
        small = dot(x_low[...], w_high[...]) + dot(x_high[...], w_low[...])
        product = dot(x_high[...], w_high[...]) + small
        scale = scales[pl.ds(p, 1), :]
        total = squares[p]
        first = part * owners
        for b in range(product.shape[1] // LANES):
            value = product[:, b * LANES : (b + 1) * LANES] * scale
            total = total + jnp.sum((value * value).reshape(rows // TILE_S, TILE_S, LANES), axis=0)
            if b < groups:
                send_main[pl.ds(first, owners), b, p, :, :] = value.reshape(owners, span, LANES)
            else:
                rest_rows[pl.ds(first * span * pair_rows + p, rows, stride=pair_rows), :] = value
        squares[p] = total

        @pl.when(step == 0)
        def _():
            pl.semaphore_wait(barrier, n - 1)

        for early in range(EARLY):
            for h in range(PARTS):
                @pl.when(step == early * PARTS + h)
                def _():
                    send(early, h * owners, (h + 1) * owners)

        return carry

    lax.fori_loop(0, PARTS * pair_rows, compute, 0)

    lane = lax.broadcasted_iota(jnp.int32, (pair_rows, LANES), 1)

    def pack(c, carry):
        packed = [jnp.zeros((pair_rows, LANES), jnp.float32)] * (span * rest // LANES)
        for s in range(span):
            at, offset = divmod(s * rest, LANES)
            value = rest_rows[pl.ds(pl.multiple_of((c * span + s) * pair_rows, pair_rows), pair_rows), :]
            if offset:
                value = pltpu.roll(value, offset, axis=1)
            if offset + rest > LANES:
                packed[at] = jnp.where(lane >= offset, value, packed[at])
                packed[at + 1] = jnp.where(lane < offset, value, packed[at + 1])
            else:
                packed[at] = jnp.where(lane >= offset, value, packed[at])
        for b, value in enumerate(packed):
            send_rest[c, :, b * LANES : (b + 1) * LANES] = value
        return carry

    lax.fori_loop(0, n, pack, 0)
    pair_lane = lax.broadcasted_iota(jnp.int32, (1, pairs), 1) - my_pair
    total = jnp.zeros((1, pairs), jnp.float32)
    for p in range(pair_rows):
        value = jnp.sum(jnp.sum(squares[p], axis=0, keepdims=True), axis=1, keepdims=True)
        total = jnp.where(pair_lane == p, value, total)
    sq_send[...] = total

    def sq_copy(dst):
        return pltpu.make_async_remote_copy(
            src_ref=sq_send, dst_ref=sq_recv.at[me],
            send_sem=sq_sems.at[0], recv_sem=sq_sems.at[1],
            device_id={"wide": dst}, device_id_type=MESH,
        )

    def send_squares(j, carry):
        sq_copy(lax.rem(me + j, n)).start()
        return carry

    for i in range(EARLY, len(sets)):
        send(i, 0, n)
        if i == EARLY:
            lax.fori_loop(1, n, send_squares, 0)
    sq_recv[me] = sq_send[...]
    recv_main[:, pl.ds(my_pair, pair_rows), :span, :] = send_main[own]
    recv_rest[pl.ds(my_pair, pair_rows), :] = send_rest[own]

    last = len(sets) - 1
    for i, (kind, at) in enumerate(sets):
        if i == last:
            others = sq_recv.at[pl.ds(0, n - 1)]
            pltpu.make_async_copy(others, others, sq_sems.at[0]).wait()
            pltpu.make_async_copy(others, others, sq_sems.at[1]).wait()
            for k in range(last):
                wait_all(k, False)
        wait_all(i, True)
        if kind == "rest":
            for b in range(at * wide * rest // LANES, (at + 1) * wide * rest // LANES):
                for q in range(pairs // LANES):
                    rest_turned[b * LANES : (b + 1) * LANES, q * LANES : (q + 1) * LANES] = (
                        recv_rest[q * LANES : (q + 1) * LANES, b * LANES : (b + 1) * LANES].T
                    )
        elif kind == "main" and i < last:
            def row(k, carry):
                assemble(recv_main, rest_turned, out_ref, at * TILE_S + k, at * TILE_S + k)
                return carry

            lax.fori_loop(0, TILE_S, row, 0)
    wait_all(last, False)


def assemble(recv_main, rest_turned, out_ref, s, to):
    groups, pairs, stride, _ = recv_main.shape
    full = groups * LANES
    rest = out_ref.shape[1] - full
    lines = recv_main.reshape(groups * pairs * stride, LANES)
    for b in range(groups):
        for q in range(pairs // LANES):
            first = (b * pairs + q * LANES) * stride + s
            out_ref[to, b * LANES : (b + 1) * LANES, q * LANES : (q + 1) * LANES] = (
                lines[pl.ds(first, LANES, stride=stride), :].T
            )
    out_ref[to, full:, :] = rest_turned[pl.ds(pl.multiple_of(s * rest, 8), rest), :]


def finish_kernel(count, main_ref, recv_main, rest_turned, sq_ref, out_ref, rms_ref, tail, rms, sems, tail_sems):
    done = main_ref.shape[0]
    copies = [
        pltpu.make_async_copy(main_ref.at[pl.ds(k, TILE_S)], out_ref.at[pl.ds(k, TILE_S)], sems.at[k // TILE_S])
        for k in range(0, done, TILE_S)
    ]
    for copy in copies:
        copy.start()
    totals = jnp.sum(sq_ref[...], axis=0)
    rms[...] = jnp.sqrt(totals / count + 1e-06)
    rms_copy = pltpu.make_async_copy(rms, rms_ref, tail_sems.at[tail.shape[0]])
    rms_copy.start()
    copies.append(rms_copy)
    for k in range(tail.shape[0]):
        assemble(recv_main, rest_turned, tail, done + k, k)
        copy = pltpu.make_async_copy(tail.at[k], out_ref.at[done + k], tail_sems.at[k])
        copy.start()
        copies.append(copy)
    for copy in copies:
        copy.wait()


def shards(n, half_integrals, pair_list, occupied_energy, virtual_orbitals, tile_order):
    pair_rows, columns, basis = half_integrals.shape
    virtuals = virtual_orbitals.shape[1]
    pairs = n * pair_rows
    span = columns // n
    deep = round_up(basis, LANES)
    broad = round_up(virtuals, LANES)
    full = virtuals // LANES * LANES
    rest = virtuals - full
    groups = full // LANES
    count = len(schedule(span, rest)[1])
    flops = 6 * pair_rows * columns * basis * virtuals
    vmem = pl.BlockSpec(memory_space=pltpu.VMEM)
    anywhere = pl.BlockSpec(memory_space=pl.ANY)

    def hbm(value):
        return pltpu.with_memory_space_constraint(value, pltpu.HBM)

    main, recv_main, rest_turned, sq_recv = pl.pallas_call(
        functools.partial(exchange_kernel, n, rest),
        out_shape=(
            pltpu.VMEM((span - TILE_S, virtuals, pairs), jnp.float32),
            pltpu.VMEM((groups, pairs, span + TILE_S, LANES), jnp.float32),
            pltpu.VMEM((span * rest, pairs), jnp.float32),
            pltpu.VMEM((n, 1, pairs), jnp.float32),
        ),
        in_specs=[anywhere] * 5,
        out_specs=(vmem,) * 4,
        scratch_shapes=[
            pltpu.SMEM(tile_order.shape, jnp.int32),
            pltpu.VMEM((2, pairs), jnp.int32),
            pltpu.VMEM((1, occupied_energy.shape[0]), jnp.float32),
            pltpu.VMEM((pairs, LANES), jnp.float32),
            pltpu.VMEM((basis, virtuals), jnp.float32),
            pltpu.VMEM((pair_rows, basis, columns), jnp.float32),
            pltpu.VMEM((columns, deep), jnp.float32),
            pltpu.VMEM((columns // PARTS, deep), jnp.bfloat16),
            pltpu.VMEM((columns // PARTS, deep), jnp.bfloat16),
            pltpu.VMEM((deep, broad), jnp.bfloat16),
            pltpu.VMEM((deep, broad), jnp.bfloat16),
            pltpu.VMEM((pair_rows, LANES), jnp.float32),
            pltpu.VMEM((pair_rows, TILE_S, LANES), jnp.float32),
            pltpu.VMEM((n, groups, pair_rows, span, LANES), jnp.float32),
            pltpu.VMEM((columns * pair_rows, LANES), jnp.float32),
            pltpu.VMEM((n, pair_rows, span * rest), jnp.float32),
            pltpu.VMEM((1, pairs), jnp.float32),
            pltpu.VMEM((pairs, span * rest), jnp.float32),
            pltpu.SemaphoreType.DMA((3,)),
            pltpu.SemaphoreType.DMA((1,)),
            pltpu.SemaphoreType.DMA((AHEAD,)),
            pltpu.SemaphoreType.DMA((count,)),
            pltpu.SemaphoreType.DMA((count,)),
            pltpu.SemaphoreType.DMA((2,)),
        ],
        compiler_params=pltpu.CompilerParams(
            collective_id=0, has_side_effects=True, vmem_limit_bytes=42 * 1024 * 1024
        ),
        cost_estimate=pl.CostEstimate(flops=flops, bytes_accessed=4 * half_integrals.size, transcendentals=0),
        name="exchange",
    )(
        hbm(tile_order), hbm(pair_list.T), hbm(occupied_energy.reshape(1, -1)),
        hbm(jnp.swapaxes(half_integrals, 1, 2)), hbm(virtual_orbitals),
    )
    out, rms = pl.pallas_call(
        functools.partial(finish_kernel, columns * virtuals),
        out_shape=(
            jax.ShapeDtypeStruct((span, virtuals, pairs), jnp.float32),
            jax.ShapeDtypeStruct((1, pairs), jnp.float32),
        ),
        in_specs=[vmem] * 4,
        out_specs=(pl.BlockSpec(memory_space=pltpu.HBM),) * 2,
        scratch_shapes=[
            pltpu.VMEM((TILE_S, virtuals, pairs), jnp.float32),
            pltpu.VMEM((1, pairs), jnp.float32),
            pltpu.SemaphoreType.DMA((span // TILE_S - 1,)),
            pltpu.SemaphoreType.DMA((TILE_S + 1,)),
        ],
        compiler_params=pltpu.CompilerParams(vmem_limit_bytes=8 * 1024 * 1024),
        name="finish",
    )(main, recv_main, rest_turned, sq_recv)
    return (jnp.transpose(out, (2, 0, 1)), rms.reshape(-1))


def solution(mesh):
    in_specs = (
        P(("groups", "wide"), None, None),
        P("groups", None),
        P("groups"),
        P("groups", None),
        P(),
    )
    out_specs = (P("groups", "wide", None), P("groups"))
    return jax.shard_map(
        functools.partial(shards, mesh.shape["wide"]),
        mesh=mesh, in_specs=in_specs, out_specs=out_specs, check_vma=False,
    )
```

```python
import functools
import math

import jax
import jax.numpy as jnp
from jax import lax
from jax.experimental import pallas as pl
from jax.experimental.pallas import tpu as pltpu
from jax.sharding import PartitionSpec as P

TILE_S = 8
LANES = 128
EARLY = 2
PARTS = 4
MESH = pl.DeviceIdType.MESH


def round_up(value, step):
    return (value + step - 1) // step * step


def split(value):
    high = value.astype(jnp.bfloat16)
    low = (value - high.astype(jnp.float32)).astype(jnp.bfloat16)
    return high, low


def schedule(span, rest):
    wide = LANES // math.gcd(rest, LANES)
    sets = [("pair", p) for p in range(EARLY)]
    for g in range(span // wide):
        sets.append(("rest", g))
        sets += [("main", g * wide // TILE_S + k) for k in range(wide // TILE_S)]
    return wide, sets


def exchange_kernel(
    n, rest, order_hbm, pair_hbm, energy_hbm, x_hbm, w_hbm, out_ref, recv_main, rest_turned, sq_recv,
    order_ref, pair_ref, energy_ref, index_buf, w_buf, x_buf, turned, x_high, x_low, w_high, w_low, scales, squares,
    send_main, rest_rows, send_rest, sq_send, recv_rest,
    small_sems, w_sem, x_sem, send_sems, recv_sems, sq_sems,
):
    me = lax.axis_index("wide")
    pair_rows, basis, columns = x_hbm.shape
    virtuals = w_hbm.shape[1]
    pairs = recv_main.shape[1]
    span = columns // n
    full = virtuals - rest
    deep = turned.shape[1]
    groups = full // LANES
    plane = n // 4
    half = n // 2
    owners = n // PARTS
    rows = owners * span
    own = 3 * plane
    owner_tiles = span // TILE_S
    stride = recv_main.shape[2]
    wide, sets = schedule(span, rest)
    late = pair_rows - EARLY
    my_pair = pl.multiple_of(me * pair_rows, pair_rows)

    barrier = pltpu.get_barrier_semaphore()

    def greet(j, carry):
        pl.semaphore_signal(barrier, inc=1, device_id={"wide": lax.rem(me + j, n)}, device_id_type=MESH)
        return carry

    small = [
        pltpu.make_async_copy(order_hbm, order_ref, small_sems.at[0]),
        pltpu.make_async_copy(pair_hbm, pair_ref, small_sems.at[1]),
        pltpu.make_async_copy(energy_hbm, energy_ref, small_sems.at[2]),
    ]
    weights_copy = pltpu.make_async_copy(w_hbm, w_buf, w_sem.at[0])

    def fetch(p):
        return pltpu.make_async_copy(x_hbm.at[p], x_buf.at[p], x_sem.at[0])

    weights_copy.start()
    for copy in small:
        copy.start()
    fetch(0).start()
    lax.fori_loop(1, n, greet, 0, unroll=5)

    sign = 1 - 2 * (me // half)
    my_plane = me // plane
    inner = jnp.minimum(my_plane, 3 - my_plane)

    def place(c):
        rank = c // plane
        away = 3 - rank - inner * jnp.where(rank < 2, 1, 6 - 2 * rank)
        return (my_plane + sign * away) * plane + lax.rem(me + c, plane)

    squares[...] = jnp.zeros_like(squares)
    w_high[...] = jnp.zeros_like(w_high)
    w_low[...] = jnp.zeros_like(w_low)
    for copy in small:
        copy.wait()
    orbitals = energy_ref.shape[1]
    orbital = lax.broadcasted_iota(jnp.int32, (pair_rows, orbitals), 1).astype(jnp.float32)
    energy = jnp.zeros((pair_rows, 1), jnp.float32)
    for k in range(2):
        line = pair_ref[k : k + 1, :].astype(jnp.float32)
        index_buf[...] = jnp.broadcast_to(line, (LANES, pairs)).T
        hit = index_buf[pl.ds(my_pair, pair_rows), 0:1] == orbital
        energy = energy + jnp.sum(jnp.where(hit, energy_ref[...], 0.0), axis=1, keepdims=True)
    scales[...] = jnp.broadcast_to(jnp.exp(0.3 * energy), scales.shape)
    weights_copy.wait()
    high, low = split(w_buf[...])
    w_high[:basis, :virtuals] = high
    w_low[:basis, :virtuals] = low

    def remote(i, c, owner):
        kind, at = sets[i]
        if kind == "pair":
            src = send_main.at[c, :, at, :, :]
            dst = recv_main.at[:, my_pair + at, pl.ds(0, span), :]
        elif kind == "main":
            src = send_main.at[c, :, pl.ds(EARLY, late), pl.ds(at * TILE_S, TILE_S), :]
            dst = recv_main.at[:, pl.ds(my_pair + EARLY, late), pl.ds(at * TILE_S, TILE_S), :]
        else:
            lanes = pl.ds(at * wide * rest, wide * rest)
            src = send_rest.at[c, :, lanes]
            dst = recv_rest.at[pl.ds(my_pair, pair_rows), lanes]
        return pltpu.make_async_remote_copy(
            src_ref=src, dst_ref=dst, send_sem=send_sems.at[i], recv_sem=recv_sems.at[i],
            device_id={"wide": owner}, device_id_type=MESH,
        )

    def wait_all(i, received):
        kind, at = sets[i]
        if kind == "pair":
            src = send_main.at[pl.ds(0, n - 1), :, at, :, :]
            dst = recv_main.at[:, pl.ds(0, n - 1), pl.ds(0, span), :]
        elif kind == "main":
            src = send_main.at[pl.ds(0, n - 1), :, pl.ds(EARLY, late), pl.ds(at * TILE_S, TILE_S), :]
            dst = recv_main.at[:, pl.ds(0, late * (n - 1)), pl.ds(at * TILE_S, TILE_S), :]
        else:
            lanes = pl.ds(at * wide * rest, wide * rest)
            src = send_rest.at[pl.ds(0, n - 1), :, lanes]
            dst = recv_rest.at[pl.ds(0, pair_rows * (n - 1)), lanes]
        ref, sem = (dst, recv_sems.at[i]) if received else (src, send_sems.at[i])
        pltpu.make_async_copy(ref, ref, sem).wait()

    def send(kinds, first, last):
        def one(c, carry):
            for i in kinds:
                remote(i, c, place(c)).start()
            return carry

        lax.fori_loop(first, min(last, own), one, 0)
        lax.fori_loop(max(first, own + 1), last, one, 0)

    def compute(step, carry):
        p = step // PARTS
        part = lax.rem(step, PARTS)

        @pl.when(part == 0)
        def _():
            fetch(p).wait()

            @pl.when(p + 1 < pair_rows)
            def _():
                fetch(p + 1).start()

            for k in range(deep // LANES):
                size = min(LANES, basis - k * LANES)
                for b in range(columns // LANES):
                    piece = x_buf[p, k * LANES : k * LANES + size, b * LANES : (b + 1) * LANES]
                    if size < LANES:
                        piece = jnp.concatenate([piece, jnp.zeros((LANES - size, LANES), jnp.float32)], axis=0)
                    turned[b * LANES : (b + 1) * LANES, k * LANES : (k + 1) * LANES] = piece.T

        def gather(u, carry):
            pieces = []
            for v in range(2):
                at = u * 2 + v
                slot = place(part * owners + at // owner_tiles) * owner_tiles + lax.rem(at, owner_tiles)
                pieces.append(turned[pl.ds(order_ref[slot] * TILE_S, TILE_S), :])
            high, low = split(jnp.concatenate(pieces, axis=0))
            block = pl.ds(pl.multiple_of(u * 2 * TILE_S, 2 * TILE_S), 2 * TILE_S)
            x_high[block, :] = high
            x_low[block, :] = low
            return carry

        lax.fori_loop(0, rows // TILE_S // 2, gather, 0, unroll=8)
        dot = functools.partial(jnp.dot, preferred_element_type=jnp.float32)
        small = dot(x_low[...], w_high[...]) + dot(x_high[...], w_low[...])
        product = dot(x_high[...], w_high[...]) + small
        scale = scales[pl.ds(p, 1), :]
        total = squares[p]
        first = part * owners
        for b in range(product.shape[1] // LANES):
            value = product[:, b * LANES : (b + 1) * LANES] * scale
            total = total + jnp.sum((value * value).reshape(rows // TILE_S, TILE_S, LANES), axis=0)
            if b < groups:
                send_main[pl.ds(first, owners), b, p, :, :] = value.reshape(owners, span, LANES)
            else:
                rest_rows[pl.ds(first * span * pair_rows + p, rows, stride=pair_rows), :] = value
        squares[p] = total

        @pl.when(step == 0)
        def _():
            pl.semaphore_wait(barrier, n - 1)

        for early in range(EARLY):
            for h in range(PARTS):
                @pl.when(step == early * PARTS + h)
                def _():
                    send([early], h * owners, (h + 1) * owners)

        return carry

    lax.fori_loop(0, PARTS * pair_rows, compute, 0)

    lane = lax.broadcasted_iota(jnp.int32, (pair_rows, LANES), 1)

    def pack(c, carry):
        packed = [jnp.zeros((pair_rows, LANES), jnp.float32)] * (span * rest // LANES)
        for s in range(span):
            at, offset = divmod(s * rest, LANES)
            value = rest_rows[pl.ds(pl.multiple_of((c * span + s) * pair_rows, pair_rows), pair_rows), :]
            if offset:
                value = pltpu.roll(value, offset, axis=1)
            if offset + rest > LANES:
                packed[at] = jnp.where(lane >= offset, value, packed[at])
                packed[at + 1] = jnp.where(lane < offset, value, packed[at + 1])
            else:
                packed[at] = jnp.where(lane >= offset, value, packed[at])
        for b, value in enumerate(packed):
            send_rest[c, :, b * LANES : (b + 1) * LANES] = value
        return carry

    lax.fori_loop(0, n, pack, 0)
    pair_lane = lax.broadcasted_iota(jnp.int32, (1, pairs), 1) - my_pair
    total = jnp.zeros((1, pairs), jnp.float32)
    for p in range(pair_rows):
        value = jnp.sum(jnp.sum(squares[p], axis=0, keepdims=True), axis=1, keepdims=True)
        total = jnp.where(pair_lane == p, value, total)
    sq_send[...] = total

    def sq_copy(dst):
        return pltpu.make_async_remote_copy(
            src_ref=sq_send, dst_ref=sq_recv.at[me],
            send_sem=sq_sems.at[0], recv_sem=sq_sems.at[1],
            device_id={"wide": dst}, device_id_type=MESH,
        )

    def send_squares(j, carry):
        sq_copy(lax.rem(me + j, n)).start()
        return carry

    last = len(sets) - 1
    lax.fori_loop(1, n, send_squares, 0)
    send(range(EARLY, last), 0, n)
    send([last], 0, n)
    sq_recv[me] = sq_send[...]
    recv_main[:, pl.ds(my_pair, pair_rows), :span, :] = send_main[own]
    recv_rest[pl.ds(my_pair, pair_rows), :] = send_rest[own]

    for i, (kind, at) in enumerate(sets):
        if i == last:
            others = sq_recv.at[pl.ds(0, n - 1)]
            pltpu.make_async_copy(others, others, sq_sems.at[0]).wait()
            pltpu.make_async_copy(others, others, sq_sems.at[1]).wait()
            for k in range(last):
                wait_all(k, False)
        wait_all(i, True)
        if kind == "rest":
            for b in range(at * wide * rest // LANES, (at + 1) * wide * rest // LANES):
                for q in range(pairs // LANES):
                    rest_turned[b * LANES : (b + 1) * LANES, q * LANES : (q + 1) * LANES] = (
                        recv_rest[q * LANES : (q + 1) * LANES, b * LANES : (b + 1) * LANES].T
                    )
        elif kind == "main" and i < last:
            def row(k, carry):
                assemble(recv_main, rest_turned, out_ref, at * TILE_S + k, at * TILE_S + k)
                return carry

            lax.fori_loop(0, TILE_S, row, 0)
    wait_all(last, False)


def assemble(recv_main, rest_turned, out_ref, s, to):
    groups, pairs, stride, _ = recv_main.shape
    full = groups * LANES
    rest = out_ref.shape[1] - full
    lines = recv_main.reshape(groups * pairs * stride, LANES)
    for b in range(groups):
        for q in range(pairs // LANES):
            first = (b * pairs + q * LANES) * stride + s
            out_ref[to, b * LANES : (b + 1) * LANES, q * LANES : (q + 1) * LANES] = (
                lines[pl.ds(first, LANES, stride=stride), :].T
            )
    out_ref[to, full:, :] = rest_turned[pl.ds(pl.multiple_of(s * rest, 8), rest), :]


def finish_kernel(count, main_ref, recv_main, rest_turned, sq_ref, out_ref, rms_ref, tail, rms, sems):
    done = main_ref.shape[0]
    rows = tail.shape[0]
    pltpu.make_async_copy(main_ref, out_ref.at[pl.ds(0, done)], sems.at[0]).start()
    totals = jnp.sum(sq_ref[...], axis=0)
    rms[...] = jnp.sqrt(totals / count + 1e-06)
    pltpu.make_async_copy(rms, rms_ref, sems.at[2]).start()
    for k in range(rows):
        assemble(recv_main, rest_turned, tail, done + k, k)
        pltpu.make_async_copy(tail.at[k], out_ref.at[done + k], sems.at[1]).start()
    pltpu.make_async_copy(tail, out_ref.at[pl.ds(done, rows)], sems.at[1]).wait()
    pltpu.make_async_copy(rms, rms_ref, sems.at[2]).wait()
    pltpu.make_async_copy(main_ref, out_ref.at[pl.ds(0, done)], sems.at[0]).wait()


def shards(n, half_integrals, pair_list, occupied_energy, virtual_orbitals, tile_order):
    pair_rows, columns, basis = half_integrals.shape
    virtuals = virtual_orbitals.shape[1]
    pairs = n * pair_rows
    span = columns // n
    deep = round_up(basis, LANES)
    broad = round_up(virtuals, LANES)
    full = virtuals // LANES * LANES
    rest = virtuals - full
    groups = full // LANES
    count = len(schedule(span, rest)[1])
    flops = 6 * pair_rows * columns * basis * virtuals
    vmem = pl.BlockSpec(memory_space=pltpu.VMEM)
    anywhere = pl.BlockSpec(memory_space=pl.ANY)

    def hbm(value):
        return pltpu.with_memory_space_constraint(value, pltpu.HBM)

    main, recv_main, rest_turned, sq_recv = pl.pallas_call(
        functools.partial(exchange_kernel, n, rest),
        out_shape=(
            pltpu.VMEM((span - TILE_S, virtuals, pairs), jnp.float32),
            pltpu.VMEM((groups, pairs, span + TILE_S, LANES), jnp.float32),
            pltpu.VMEM((span * rest, pairs), jnp.float32),
            pltpu.VMEM((n, 1, pairs), jnp.float32),
        ),
        in_specs=[anywhere] * 5,
        out_specs=(vmem,) * 4,
        scratch_shapes=[
            pltpu.SMEM(tile_order.shape, jnp.int32),
            pltpu.VMEM((2, pairs), jnp.int32),
            pltpu.VMEM((1, occupied_energy.shape[0]), jnp.float32),
            pltpu.VMEM((pairs, LANES), jnp.float32),
            pltpu.VMEM((basis, virtuals), jnp.float32),
            pltpu.VMEM((pair_rows, basis, columns), jnp.float32),
            pltpu.VMEM((columns, deep), jnp.float32),
            pltpu.VMEM((columns // PARTS, deep), jnp.bfloat16),
            pltpu.VMEM((columns // PARTS, deep), jnp.bfloat16),
            pltpu.VMEM((deep, broad), jnp.bfloat16),
            pltpu.VMEM((deep, broad), jnp.bfloat16),
            pltpu.VMEM((pair_rows, LANES), jnp.float32),
            pltpu.VMEM((pair_rows, TILE_S, LANES), jnp.float32),
            pltpu.VMEM((n, groups, pair_rows, span, LANES), jnp.float32),
            pltpu.VMEM((columns * pair_rows, LANES), jnp.float32),
            pltpu.VMEM((n, pair_rows, span * rest), jnp.float32),
            pltpu.VMEM((1, pairs), jnp.float32),
            pltpu.VMEM((pairs, span * rest), jnp.float32),
            pltpu.SemaphoreType.DMA((3,)),
            pltpu.SemaphoreType.DMA((1,)),
            pltpu.SemaphoreType.DMA((1,)),
            pltpu.SemaphoreType.DMA((count,)),
            pltpu.SemaphoreType.DMA((count,)),
            pltpu.SemaphoreType.DMA((2,)),
        ],
        compiler_params=pltpu.CompilerParams(
            collective_id=0, has_side_effects=True, vmem_limit_bytes=42 * 1024 * 1024
        ),
        cost_estimate=pl.CostEstimate(flops=flops, bytes_accessed=4 * half_integrals.size, transcendentals=0),
        name="exchange",
    )(
        hbm(tile_order), hbm(pair_list.T), hbm(occupied_energy.reshape(1, -1)),
        hbm(jnp.swapaxes(half_integrals, 1, 2)), hbm(virtual_orbitals),
    )
    out, rms = pl.pallas_call(
        functools.partial(finish_kernel, columns * virtuals),
        out_shape=(
            jax.ShapeDtypeStruct((span, virtuals, pairs), jnp.float32),
            jax.ShapeDtypeStruct((1, pairs), jnp.float32),
        ),
        in_specs=[vmem] * 4,
        out_specs=(pl.BlockSpec(memory_space=pltpu.HBM),) * 2,
        scratch_shapes=[
            pltpu.VMEM((TILE_S, virtuals, pairs), jnp.float32),
            pltpu.VMEM((1, pairs), jnp.float32),
            pltpu.SemaphoreType.DMA((3,)),
        ],
        compiler_params=pltpu.CompilerParams(vmem_limit_bytes=8 * 1024 * 1024),
        name="finish",
    )(main, recv_main, rest_turned, sq_recv)
    return (jnp.transpose(out, (2, 0, 1)), rms.reshape(-1))


def solution(mesh):
    in_specs = (
        P(("groups", "wide"), None, None),
        P("groups", None),
        P("groups"),
        P("groups", None),
        P(),
    )
    out_specs = (P("groups", "wide", None), P("groups"))
    return jax.shard_map(
        functools.partial(shards, mesh.shape["wide"]),
        mesh=mesh, in_specs=in_specs, out_specs=out_specs, check_vma=False,
    )
```

```python
import functools
import math

import jax
import jax.numpy as jnp
from jax import lax
from jax.experimental import pallas as pl
from jax.experimental.pallas import tpu as pltpu
from jax.sharding import PartitionSpec as P

TILE_S = 8
LANES = 128
EARLY = 2
PARTS = 4
MESH = pl.DeviceIdType.MESH


def round_up(value, step):
    return (value + step - 1) // step * step


def split(value):
    high = value.astype(jnp.bfloat16)
    low = (value - high.astype(jnp.float32)).astype(jnp.bfloat16)
    return high, low


def schedule(span, rest):
    wide = LANES // math.gcd(rest, LANES)
    sets = [("pair", p) for p in range(EARLY)]
    for g in range(span // wide):
        sets.append(("rest", g))
        sets += [("main", g * wide // TILE_S + k) for k in range(wide // TILE_S)]
    return wide, sets


def exchange_kernel(
    n, rest, order_hbm, pair_hbm, energy_hbm, x_hbm, w_hbm, out_ref, recv_main, rest_turned, sq_recv,
    order_ref, pair_ref, energy_ref, index_buf, w_buf, x_buf, turned, x_high, x_low, w_high, w_low, scales, squares,
    send_main, rest_rows, send_rest, sq_send, recv_rest,
    small_sems, w_sem, x_sem, send_sems, recv_sems, sq_sems,
):
    me = lax.axis_index("wide")
    pair_rows, basis, columns = x_hbm.shape
    virtuals = w_hbm.shape[1]
    pairs = recv_main.shape[1]
    span = columns // n
    full = virtuals - rest
    deep = turned.shape[1]
    groups = full // LANES
    plane = n // 4
    half = n // 2
    owners = n // PARTS
    rows = owners * span
    own = 3 * plane
    owner_tiles = span // TILE_S
    stride = recv_main.shape[2]
    wide, sets = schedule(span, rest)
    late = pair_rows - EARLY
    my_pair = pl.multiple_of(me * pair_rows, pair_rows)

    barrier = pltpu.get_barrier_semaphore()

    def greet(j, carry):
        pl.semaphore_signal(barrier, inc=1, device_id={"wide": lax.rem(me + j, n)}, device_id_type=MESH)
        return carry

    small = [
        pltpu.make_async_copy(order_hbm, order_ref, small_sems.at[0]),
        pltpu.make_async_copy(pair_hbm, pair_ref, small_sems.at[1]),
        pltpu.make_async_copy(energy_hbm, energy_ref, small_sems.at[2]),
    ]
    weights_copy = pltpu.make_async_copy(w_hbm, w_buf, w_sem.at[0])

    def fetch(p):
        return pltpu.make_async_copy(x_hbm.at[p], x_buf.at[p], x_sem.at[0])

    weights_copy.start()
    for copy in small:
        copy.start()
    fetch(0).start()
    lax.fori_loop(1, n, greet, 0, unroll=5)

    sign = 1 - 2 * (me // half)
    my_plane = me // plane
    inner = jnp.minimum(my_plane, 3 - my_plane)

    def place(c):
        rank = c // plane
        away = 3 - rank - inner * jnp.where(rank < 2, 1, 6 - 2 * rank)
        return (my_plane + sign * away) * plane + lax.rem(me + c, plane)

    squares[...] = jnp.zeros_like(squares)
    w_high[...] = jnp.zeros_like(w_high)
    w_low[...] = jnp.zeros_like(w_low)
    for copy in small:
        copy.wait()
    orbitals = energy_ref.shape[1]
    orbital = lax.broadcasted_iota(jnp.int32, (pair_rows, orbitals), 1).astype(jnp.float32)
    energy = jnp.zeros((pair_rows, 1), jnp.float32)
    for k in range(2):
        line = pair_ref[k : k + 1, :].astype(jnp.float32)
        index_buf[...] = jnp.broadcast_to(line, (LANES, pairs)).T
        hit = index_buf[pl.ds(my_pair, pair_rows), 0:1] == orbital
        energy = energy + jnp.sum(jnp.where(hit, energy_ref[...], 0.0), axis=1, keepdims=True)
    scales[...] = jnp.broadcast_to(jnp.exp(0.3 * energy), scales.shape)
    weights_copy.wait()
    high, low = split(w_buf[...])
    w_high[:basis, :virtuals] = high
    w_low[:basis, :virtuals] = low

    def remote(i, c, owner):
        kind, at = sets[i]
        if kind == "pair":
            src = send_main.at[c, :, at, :, :]
            dst = recv_main.at[:, my_pair + at, pl.ds(0, span), :]
        elif kind == "main":
            src = send_main.at[c, :, pl.ds(EARLY, late), pl.ds(at * TILE_S, TILE_S), :]
            dst = recv_main.at[:, pl.ds(my_pair + EARLY, late), pl.ds(at * TILE_S, TILE_S), :]
        else:
            lanes = pl.ds(at * wide * rest, wide * rest)
            src = send_rest.at[c, :, lanes]
            dst = recv_rest.at[pl.ds(my_pair, pair_rows), lanes]
        return pltpu.make_async_remote_copy(
            src_ref=src, dst_ref=dst, send_sem=send_sems.at[i], recv_sem=recv_sems.at[i],
            device_id={"wide": owner}, device_id_type=MESH,
        )

    def wait_all(i, received):
        kind, at = sets[i]
        if kind == "pair":
            src = send_main.at[pl.ds(0, n - 1), :, at, :, :]
            dst = recv_main.at[:, pl.ds(0, n - 1), pl.ds(0, span), :]
        elif kind == "main":
            src = send_main.at[pl.ds(0, n - 1), :, pl.ds(EARLY, late), pl.ds(at * TILE_S, TILE_S), :]
            dst = recv_main.at[:, pl.ds(0, late * (n - 1)), pl.ds(at * TILE_S, TILE_S), :]
        else:
            lanes = pl.ds(at * wide * rest, wide * rest)
            src = send_rest.at[pl.ds(0, n - 1), :, lanes]
            dst = recv_rest.at[pl.ds(0, pair_rows * (n - 1)), lanes]
        ref, sem = (dst, recv_sems.at[i]) if received else (src, send_sems.at[i])
        pltpu.make_async_copy(ref, ref, sem).wait()

    def send(kinds, first, last):
        def one(c, carry):
            for i in kinds:
                remote(i, c, place(c)).start()
            return carry

        lax.fori_loop(first, min(last, own), one, 0)
        lax.fori_loop(max(first, own + 1), last, one, 0)

    def compute(step, carry):
        p = step // PARTS
        part = lax.rem(step, PARTS)

        @pl.when(part == 0)
        def _():
            fetch(p).wait()

            @pl.when(p + 1 < pair_rows)
            def _():
                fetch(p + 1).start()

            for k in range(deep // LANES):
                size = min(LANES, basis - k * LANES)
                for b in range(columns // LANES):
                    piece = x_buf[p, k * LANES : k * LANES + size, b * LANES : (b + 1) * LANES]
                    if size < LANES:
                        piece = jnp.concatenate([piece, jnp.zeros((LANES - size, LANES), jnp.float32)], axis=0)
                    turned[b * LANES : (b + 1) * LANES, k * LANES : (k + 1) * LANES] = piece.T

        def gather(u, carry):
            pieces = []
            for v in range(2):
                at = u * 2 + v
                slot = place(part * owners + at // owner_tiles) * owner_tiles + lax.rem(at, owner_tiles)
                pieces.append(turned[pl.ds(order_ref[slot] * TILE_S, TILE_S), :])
            high, low = split(jnp.concatenate(pieces, axis=0))
            block = pl.ds(pl.multiple_of(u * 2 * TILE_S, 2 * TILE_S), 2 * TILE_S)
            x_high[block, :] = high
            x_low[block, :] = low
            return carry

        lax.fori_loop(0, rows // TILE_S // 2, gather, 0, unroll=8)
        dot = functools.partial(jnp.dot, preferred_element_type=jnp.float32)
        small = dot(x_low[...], w_high[...]) + dot(x_high[...], w_low[...])
        product = dot(x_high[...], w_high[...]) + small
        scale = scales[pl.ds(p, 1), :]
        total = squares[p]
        first = part * owners
        for b in range(product.shape[1] // LANES):
            value = product[:, b * LANES : (b + 1) * LANES] * scale
            total = total + jnp.sum((value * value).reshape(rows // TILE_S, TILE_S, LANES), axis=0)
            if b < groups:
                send_main[pl.ds(first, owners), b, p, :, :] = value.reshape(owners, span, LANES)
            else:
                rest_rows[pl.ds(first * span * pair_rows + p, rows, stride=pair_rows), :] = value
        squares[p] = total

        @pl.when(step == 0)
        def _():
            pl.semaphore_wait(barrier, n - 1)

        for early in range(EARLY):
            for h in range(PARTS):
                @pl.when(step == early * PARTS + h)
                def _():
                    send([early], h * owners, (h + 1) * owners)

        return carry

    lax.fori_loop(0, PARTS * pair_rows, compute, 0)

    lane = lax.broadcasted_iota(jnp.int32, (pair_rows, LANES), 1)

    def pack(c, carry):
        packed = [jnp.zeros((pair_rows, LANES), jnp.float32)] * (span * rest // LANES)
        for s in range(span):
            at, offset = divmod(s * rest, LANES)
            value = rest_rows[pl.ds(pl.multiple_of((c * span + s) * pair_rows, pair_rows), pair_rows), :]
            if offset:
                value = pltpu.roll(value, offset, axis=1)
            if offset + rest > LANES:
                packed[at] = jnp.where(lane >= offset, value, packed[at])
                packed[at + 1] = jnp.where(lane < offset, value, packed[at + 1])
            else:
                packed[at] = jnp.where(lane >= offset, value, packed[at])
        for b, value in enumerate(packed):
            send_rest[c, :, b * LANES : (b + 1) * LANES] = value
        return carry

    lax.fori_loop(0, n, pack, 0)
    pair_lane = lax.broadcasted_iota(jnp.int32, (1, pairs), 1) - my_pair
    total = jnp.zeros((1, pairs), jnp.float32)
    for p in range(pair_rows):
        value = jnp.sum(jnp.sum(squares[p], axis=0, keepdims=True), axis=1, keepdims=True)
        total = jnp.where(pair_lane == p, value, total)
    sq_send[...] = total

    def sq_copy(dst):
        return pltpu.make_async_remote_copy(
            src_ref=sq_send, dst_ref=sq_recv.at[me],
            send_sem=sq_sems.at[0], recv_sem=sq_sems.at[1],
            device_id={"wide": dst}, device_id_type=MESH,
        )

    def send_squares(j, carry):
        sq_copy(lax.rem(me + j, n)).start()
        return carry

    last = len(sets) - 1
    lax.fori_loop(1, n, send_squares, 0)
    send(range(EARLY, last), 0, n)
    send([last], 0, n)
    sq_recv[me] = sq_send[...]
    recv_main[:, pl.ds(my_pair, pair_rows), :span, :] = send_main[own]
    recv_rest[pl.ds(my_pair, pair_rows), :] = send_rest[own]

    for i, (kind, at) in enumerate(sets):
        if i == last:
            others = sq_recv.at[pl.ds(0, n - 1)]
            pltpu.make_async_copy(others, others, sq_sems.at[0]).wait()
            pltpu.make_async_copy(others, others, sq_sems.at[1]).wait()
            for k in range(last):
                wait_all(k, False)
        wait_all(i, True)
        if kind == "rest":
            for b in range(at * wide * rest // LANES, (at + 1) * wide * rest // LANES):
                for q in range(pairs // LANES):
                    rest_turned[b * LANES : (b + 1) * LANES, q * LANES : (q + 1) * LANES] = (
                        recv_rest[q * LANES : (q + 1) * LANES, b * LANES : (b + 1) * LANES].T
                    )
        elif kind == "main" and i < last:
            def row(k, carry):
                assemble(recv_main, rest_turned, out_ref, at * TILE_S + k, at * TILE_S + k)
                return carry

            lax.fori_loop(0, TILE_S, row, 0)
    wait_all(last, False)


def assemble(recv_main, rest_turned, out_ref, s, to):
    groups, pairs, stride, _ = recv_main.shape
    full = groups * LANES
    rest = out_ref.shape[1] - full
    lines = recv_main.reshape(groups * pairs * stride, LANES)
    for b in range(groups):
        for q in range(pairs // LANES):
            first = (b * pairs + q * LANES) * stride + s
            out_ref[to, b * LANES : (b + 1) * LANES, q * LANES : (q + 1) * LANES] = (
                lines[pl.ds(first, LANES, stride=stride), :].T
            )
    out_ref[to, full:, :] = rest_turned[pl.ds(pl.multiple_of(s * rest, 8), rest), :]


def finish_kernel(count, main_ref, recv_main, rest_turned, sq_ref, out_ref, rms_ref, tail, rms, sems):
    done = main_ref.shape[0]
    rows = tail.shape[0]
    pltpu.make_async_copy(main_ref, out_ref.at[pl.ds(0, done)], sems.at[0]).start()
    totals = jnp.sum(sq_ref[...], axis=0)
    rms[...] = jnp.sqrt(totals / count + 1e-06)
    pltpu.make_async_copy(rms, rms_ref, sems.at[2]).start()
    def write(k):
        return pltpu.make_async_copy(tail.at[k], out_ref.at[done + k], sems.at[1])

    for k in range(rows):
        assemble(recv_main, rest_turned, tail, done + k, k)
        if k:
            write(k - 1).start()
    write(rows - 1).start()
    pltpu.make_async_copy(tail, out_ref.at[pl.ds(done, rows)], sems.at[1]).wait()
    pltpu.make_async_copy(rms, rms_ref, sems.at[2]).wait()
    pltpu.make_async_copy(main_ref, out_ref.at[pl.ds(0, done)], sems.at[0]).wait()


def shards(n, half_integrals, pair_list, occupied_energy, virtual_orbitals, tile_order):
    pair_rows, columns, basis = half_integrals.shape
    virtuals = virtual_orbitals.shape[1]
    pairs = n * pair_rows
    span = columns // n
    deep = round_up(basis, LANES)
    broad = round_up(virtuals, LANES)
    full = virtuals // LANES * LANES
    rest = virtuals - full
    groups = full // LANES
    count = len(schedule(span, rest)[1])
    flops = 6 * pair_rows * columns * basis * virtuals
    vmem = pl.BlockSpec(memory_space=pltpu.VMEM)
    anywhere = pl.BlockSpec(memory_space=pl.ANY)

    def hbm(value):
        return pltpu.with_memory_space_constraint(value, pltpu.HBM)

    main, recv_main, rest_turned, sq_recv = pl.pallas_call(
        functools.partial(exchange_kernel, n, rest),
        out_shape=(
            pltpu.VMEM((span - TILE_S, virtuals, pairs), jnp.float32),
            pltpu.VMEM((groups, pairs, span + TILE_S, LANES), jnp.float32),
            pltpu.VMEM((span * rest, pairs), jnp.float32),
            pltpu.VMEM((n, 1, pairs), jnp.float32),
        ),
        in_specs=[anywhere] * 5,
        out_specs=(vmem,) * 4,
        scratch_shapes=[
            pltpu.SMEM(tile_order.shape, jnp.int32),
            pltpu.VMEM((2, pairs), jnp.int32),
            pltpu.VMEM((1, occupied_energy.shape[0]), jnp.float32),
            pltpu.VMEM((pairs, LANES), jnp.float32),
            pltpu.VMEM((basis, virtuals), jnp.float32),
            pltpu.VMEM((pair_rows, basis, columns), jnp.float32),
            pltpu.VMEM((columns, deep), jnp.float32),
            pltpu.VMEM((columns // PARTS, deep), jnp.bfloat16),
            pltpu.VMEM((columns // PARTS, deep), jnp.bfloat16),
            pltpu.VMEM((deep, broad), jnp.bfloat16),
            pltpu.VMEM((deep, broad), jnp.bfloat16),
            pltpu.VMEM((pair_rows, LANES), jnp.float32),
            pltpu.VMEM((pair_rows, TILE_S, LANES), jnp.float32),
            pltpu.VMEM((n, groups, pair_rows, span, LANES), jnp.float32),
            pltpu.VMEM((columns * pair_rows, LANES), jnp.float32),
            pltpu.VMEM((n, pair_rows, span * rest), jnp.float32),
            pltpu.VMEM((1, pairs), jnp.float32),
            pltpu.VMEM((pairs, span * rest), jnp.float32),
            pltpu.SemaphoreType.DMA((3,)),
            pltpu.SemaphoreType.DMA((1,)),
            pltpu.SemaphoreType.DMA((1,)),
            pltpu.SemaphoreType.DMA((count,)),
            pltpu.SemaphoreType.DMA((count,)),
            pltpu.SemaphoreType.DMA((2,)),
        ],
        compiler_params=pltpu.CompilerParams(
            collective_id=0, has_side_effects=True, vmem_limit_bytes=42 * 1024 * 1024
        ),
        cost_estimate=pl.CostEstimate(flops=flops, bytes_accessed=4 * half_integrals.size, transcendentals=0),
        name="exchange",
    )(
        hbm(tile_order), hbm(pair_list.T), hbm(occupied_energy.reshape(1, -1)),
        hbm(jnp.swapaxes(half_integrals, 1, 2)), hbm(virtual_orbitals),
    )
    out, rms = pl.pallas_call(
        functools.partial(finish_kernel, columns * virtuals),
        out_shape=(
            jax.ShapeDtypeStruct((span, virtuals, pairs), jnp.float32),
            jax.ShapeDtypeStruct((1, pairs), jnp.float32),
        ),
        in_specs=[vmem] * 4,
        out_specs=(pl.BlockSpec(memory_space=pltpu.HBM),) * 2,
        scratch_shapes=[
            pltpu.VMEM((TILE_S, virtuals, pairs), jnp.float32),
            pltpu.VMEM((1, pairs), jnp.float32),
            pltpu.SemaphoreType.DMA((3,)),
        ],
        compiler_params=pltpu.CompilerParams(vmem_limit_bytes=8 * 1024 * 1024),
        name="finish",
    )(main, recv_main, rest_turned, sq_recv)
    return (jnp.transpose(out, (2, 0, 1)), rms.reshape(-1))


def solution(mesh):
    in_specs = (
        P(("groups", "wide"), None, None),
        P("groups", None),
        P("groups"),
        P("groups", None),
        P(),
    )
    out_specs = (P("groups", "wide", None), P("groups"))
    return jax.shard_map(
        functools.partial(shards, mesh.shape["wide"]),
        mesh=mesh, in_specs=in_specs, out_specs=out_specs, check_vma=False,
    )
```

```python
import functools
import math

import jax
import jax.numpy as jnp
from jax import lax
from jax.experimental import pallas as pl
from jax.experimental.pallas import tpu as pltpu
from jax.sharding import PartitionSpec as P

TILE_S = 8
LANES = 128
EARLY = 3
PARTS = 4
MESH = pl.DeviceIdType.MESH


def round_up(value, step):
    return (value + step - 1) // step * step


def split(value):
    high = value.astype(jnp.bfloat16)
    low = (value - high.astype(jnp.float32)).astype(jnp.bfloat16)
    return high, low


def schedule(span, rest):
    wide = LANES // math.gcd(rest, LANES)
    sets = [("pair", p) for p in range(EARLY)]
    for g in range(span // wide):
        sets.append(("rest", g))
        sets += [("main", g * wide // TILE_S + k) for k in range(wide // TILE_S)]
    return wide, sets


def exchange_kernel(
    n, rest, order_hbm, pair_hbm, energy_hbm, x_hbm, w_hbm, out_ref, recv_main, rest_turned, sq_recv,
    order_ref, pair_ref, energy_ref, index_buf, w_buf, x_buf, turned, x_split, w_split, scales, squares,
    send_main, rest_rows, send_rest, sq_send, recv_rest,
    small_sems, w_sem, x_sem, send_sems, recv_sems, sq_sems,
):
    me = lax.axis_index("wide")
    pair_rows, basis, columns = x_hbm.shape
    virtuals = w_hbm.shape[1]
    pairs = recv_main.shape[1]
    span = columns // n
    full = virtuals - rest
    deep = turned.shape[1]
    groups = full // LANES
    plane = n // 4
    half = n // 2
    owners = n // PARTS
    rows = owners * span
    own = 3 * plane
    owner_tiles = span // TILE_S
    stride = recv_main.shape[2]
    wide, sets = schedule(span, rest)
    late = pair_rows - EARLY
    my_pair = pl.multiple_of(me * pair_rows, pair_rows)

    barrier = pltpu.get_barrier_semaphore()

    def greet(j, carry):
        pl.semaphore_signal(barrier, inc=1, device_id={"wide": lax.rem(me + j, n)}, device_id_type=MESH)
        return carry

    small = [
        pltpu.make_async_copy(order_hbm, order_ref, small_sems.at[0]),
        pltpu.make_async_copy(pair_hbm, pair_ref, small_sems.at[1]),
        pltpu.make_async_copy(energy_hbm, energy_ref, small_sems.at[2]),
    ]
    weights_copy = pltpu.make_async_copy(w_hbm, w_buf, w_sem.at[0])

    def fetch(p):
        return pltpu.make_async_copy(x_hbm.at[p], x_buf.at[p], x_sem.at[0])

    weights_copy.start()
    for copy in small:
        copy.start()
    fetch(0).start()
    lax.fori_loop(1, n, greet, 0, unroll=5)

    sign = 1 - 2 * (me // half)
    my_plane = me // plane
    inner = jnp.minimum(my_plane, 3 - my_plane)

    def place(c):
        rank = c // plane
        away = 3 - rank - inner * jnp.where(rank < 2, 1, 6 - 2 * rank)
        return (my_plane + sign * away) * plane + lax.rem(me + c, plane)

    squares[...] = jnp.zeros_like(squares)
    w_split[...] = jnp.zeros_like(w_split)
    for copy in small:
        copy.wait()
    orbitals = energy_ref.shape[1]
    orbital = lax.broadcasted_iota(jnp.int32, (pair_rows, orbitals), 1).astype(jnp.float32)
    energy = jnp.zeros((pair_rows, 1), jnp.float32)
    for k in range(2):
        line = pair_ref[k : k + 1, :].astype(jnp.float32)
        index_buf[...] = jnp.broadcast_to(line, (LANES, pairs)).T
        hit = index_buf[pl.ds(my_pair, pair_rows), 0:1] == orbital
        energy = energy + jnp.sum(jnp.where(hit, energy_ref[...], 0.0), axis=1, keepdims=True)
    scales[...] = jnp.broadcast_to(jnp.exp(0.3 * energy), scales.shape)
    weights_copy.wait()
    high, low = split(w_buf[...])
    for k, value in enumerate((high, high, low)):
        w_split[k * deep : k * deep + basis, :virtuals] = value

    def remote(i, c, owner):
        kind, at = sets[i]
        if kind == "pair":
            src = send_main.at[c, :, at, :, :]
            dst = recv_main.at[:, my_pair + at, pl.ds(0, span), :]
        elif kind == "main":
            src = send_main.at[c, :, pl.ds(EARLY, late), pl.ds(at * TILE_S, TILE_S), :]
            dst = recv_main.at[:, pl.ds(my_pair + EARLY, late), pl.ds(at * TILE_S, TILE_S), :]
        else:
            lanes = pl.ds(at * wide * rest, wide * rest)
            src = send_rest.at[c, :, lanes]
            dst = recv_rest.at[pl.ds(my_pair, pair_rows), lanes]
        return pltpu.make_async_remote_copy(
            src_ref=src, dst_ref=dst, send_sem=send_sems.at[i], recv_sem=recv_sems.at[i],
            device_id={"wide": owner}, device_id_type=MESH,
        )

    def wait_all(i, received):
        kind, at = sets[i]
        if kind == "pair":
            src = send_main.at[pl.ds(0, n - 1), :, at, :, :]
            dst = recv_main.at[:, pl.ds(0, n - 1), pl.ds(0, span), :]
        elif kind == "main":
            src = send_main.at[pl.ds(0, n - 1), :, pl.ds(EARLY, late), pl.ds(at * TILE_S, TILE_S), :]
            dst = recv_main.at[:, pl.ds(0, late * (n - 1)), pl.ds(at * TILE_S, TILE_S), :]
        else:
            lanes = pl.ds(at * wide * rest, wide * rest)
            src = send_rest.at[pl.ds(0, n - 1), :, lanes]
            dst = recv_rest.at[pl.ds(0, pair_rows * (n - 1)), lanes]
        ref, sem = (dst, recv_sems.at[i]) if received else (src, send_sems.at[i])
        pltpu.make_async_copy(ref, ref, sem).wait()

    def send(kinds, first, last):
        def one(c, carry):
            for i in kinds:
                remote(i, c, place(c)).start()
            return carry

        lax.fori_loop(first, min(last, own), one, 0)
        lax.fori_loop(max(first, own + 1), last, one, 0)

    def compute(step, carry):
        p = step // PARTS
        part = lax.rem(step, PARTS)

        @pl.when(part == 0)
        def _():
            fetch(p).wait()

            @pl.when(p + 1 < pair_rows)
            def _():
                fetch(p + 1).start()

            for k in range(deep // LANES):
                size = min(LANES, basis - k * LANES)
                for b in range(columns // LANES):
                    piece = x_buf[p, k * LANES : k * LANES + size, b * LANES : (b + 1) * LANES]
                    if size < LANES:
                        piece = jnp.concatenate([piece, jnp.zeros((LANES - size, LANES), jnp.float32)], axis=0)
                    turned[b * LANES : (b + 1) * LANES, k * LANES : (k + 1) * LANES] = piece.T

        def gather(u, carry):
            pieces = []
            for v in range(2):
                at = u * 2 + v
                slot = place(part * owners + at // owner_tiles) * owner_tiles + lax.rem(at, owner_tiles)
                pieces.append(turned[pl.ds(order_ref[slot] * TILE_S, TILE_S), :])
            high, low = split(jnp.concatenate(pieces, axis=0))
            block = pl.ds(pl.multiple_of(u * 2 * TILE_S, 2 * TILE_S), 2 * TILE_S)
            for k, value in enumerate((high, low, high)):
                x_split[block, k * deep : (k + 1) * deep] = value
            return carry

        lax.fori_loop(0, rows // TILE_S // 2, gather, 0, unroll=8)
        product = jnp.dot(x_split[...], w_split[...], preferred_element_type=jnp.float32)
        scale = scales[pl.ds(p, 1), :]
        total = squares[p]
        first = part * owners
        for b in range(product.shape[1] // LANES):
            value = product[:, b * LANES : (b + 1) * LANES] * scale
            total = total + jnp.sum((value * value).reshape(rows // TILE_S, TILE_S, LANES), axis=0)
            if b < groups:
                send_main[pl.ds(first, owners), b, p, :, :] = value.reshape(owners, span, LANES)
            else:
                rest_rows[pl.ds(first * span * pair_rows + p, rows, stride=pair_rows), :] = value
        squares[p] = total

        @pl.when(step == 0)
        def _():
            pl.semaphore_wait(barrier, n - 1)

        for early in range(EARLY):
            for h in range(PARTS):
                @pl.when(step == early * PARTS + h)
                def _():
                    send([early], h * owners, (h + 1) * owners)

        return carry

    lax.fori_loop(0, PARTS * pair_rows, compute, 0)

    lane = lax.broadcasted_iota(jnp.int32, (pair_rows, LANES), 1)

    def pack(c, carry):
        packed = [jnp.zeros((pair_rows, LANES), jnp.float32)] * (span * rest // LANES)
        for s in range(span):
            at, offset = divmod(s * rest, LANES)
            value = rest_rows[pl.ds(pl.multiple_of((c * span + s) * pair_rows, pair_rows), pair_rows), :]
            if offset:
                value = pltpu.roll(value, offset, axis=1)
            if offset + rest > LANES:
                packed[at] = jnp.where(lane >= offset, value, packed[at])
                packed[at + 1] = jnp.where(lane < offset, value, packed[at + 1])
            else:
                packed[at] = jnp.where(lane >= offset, value, packed[at])
        for b, value in enumerate(packed):
            send_rest[c, :, b * LANES : (b + 1) * LANES] = value
        return carry

    lax.fori_loop(0, n, pack, 0)
    pair_lane = lax.broadcasted_iota(jnp.int32, (1, pairs), 1) - my_pair
    total = jnp.zeros((1, pairs), jnp.float32)
    for p in range(pair_rows):
        value = jnp.sum(jnp.sum(squares[p], axis=0, keepdims=True), axis=1, keepdims=True)
        total = jnp.where(pair_lane == p, value, total)
    sq_send[...] = total

    def sq_copy(dst):
        return pltpu.make_async_remote_copy(
            src_ref=sq_send, dst_ref=sq_recv.at[me],
            send_sem=sq_sems.at[0], recv_sem=sq_sems.at[1],
            device_id={"wide": dst}, device_id_type=MESH,
        )

    def send_squares(j, carry):
        sq_copy(lax.rem(me + j, n)).start()
        return carry

    last = len(sets) - 1
    lax.fori_loop(1, n, send_squares, 0)
    send(range(EARLY, last), 0, n)
    send([last], 0, n)
    sq_recv[me] = sq_send[...]
    recv_main[:, pl.ds(my_pair, pair_rows), :span, :] = send_main[own]
    recv_rest[pl.ds(my_pair, pair_rows), :] = send_rest[own]

    for i, (kind, at) in enumerate(sets):
        if i == last:
            others = sq_recv.at[pl.ds(0, n - 1)]
            pltpu.make_async_copy(others, others, sq_sems.at[0]).wait()
            pltpu.make_async_copy(others, others, sq_sems.at[1]).wait()
            for k in range(last):
                wait_all(k, False)
        wait_all(i, True)
        if kind == "rest":
            for b in range(at * wide * rest // LANES, (at + 1) * wide * rest // LANES):
                for q in range(pairs // LANES):
                    rest_turned[b * LANES : (b + 1) * LANES, q * LANES : (q + 1) * LANES] = (
                        recv_rest[q * LANES : (q + 1) * LANES, b * LANES : (b + 1) * LANES].T
                    )
        elif kind == "main" and i < last:
            def row(k, carry):
                assemble(recv_main, rest_turned, out_ref, at * TILE_S + k, at * TILE_S + k)
                return carry

            lax.fori_loop(0, TILE_S, row, 0)
    wait_all(last, False)


def assemble(recv_main, rest_turned, out_ref, s, to):
    groups, pairs, stride, _ = recv_main.shape
    full = groups * LANES
    rest = out_ref.shape[1] - full
    lines = recv_main.reshape(groups * pairs * stride, LANES)
    for b in range(groups):
        for q in range(pairs // LANES):
            first = (b * pairs + q * LANES) * stride + s
            out_ref[to, b * LANES : (b + 1) * LANES, q * LANES : (q + 1) * LANES] = (
                lines[pl.ds(first, LANES, stride=stride), :].T
            )
    out_ref[to, full:, :] = rest_turned[pl.ds(pl.multiple_of(s * rest, 8), rest), :]


def finish_kernel(count, main_ref, recv_main, rest_turned, sq_ref, out_ref, rms_ref, tail, rms, sems):
    done = main_ref.shape[0]
    rows = tail.shape[0]
    pltpu.make_async_copy(main_ref, out_ref.at[pl.ds(0, done)], sems.at[0]).start()
    totals = jnp.sum(sq_ref[...], axis=0)
    rms[...] = jnp.sqrt(totals / count + 1e-06)
    pltpu.make_async_copy(rms, rms_ref, sems.at[2]).start()
    def write(k):
        return pltpu.make_async_copy(tail.at[k], out_ref.at[done + k], sems.at[1])

    for k in range(rows):
        assemble(recv_main, rest_turned, tail, done + k, k)
        if k:
            write(k - 1).start()
    write(rows - 1).start()
    pltpu.make_async_copy(tail, out_ref.at[pl.ds(done, rows)], sems.at[1]).wait()
    pltpu.make_async_copy(rms, rms_ref, sems.at[2]).wait()
    pltpu.make_async_copy(main_ref, out_ref.at[pl.ds(0, done)], sems.at[0]).wait()


def shards(n, half_integrals, pair_list, occupied_energy, virtual_orbitals, tile_order):
    pair_rows, columns, basis = half_integrals.shape
    virtuals = virtual_orbitals.shape[1]
    pairs = n * pair_rows
    span = columns // n
    deep = round_up(basis, LANES)
    broad = round_up(virtuals, LANES)
    full = virtuals // LANES * LANES
    rest = virtuals - full
    groups = full // LANES
    count = len(schedule(span, rest)[1])
    flops = 6 * pair_rows * columns * basis * virtuals
    vmem = pl.BlockSpec(memory_space=pltpu.VMEM)
    anywhere = pl.BlockSpec(memory_space=pl.ANY)

    def hbm(value):
        return pltpu.with_memory_space_constraint(value, pltpu.HBM)

    main, recv_main, rest_turned, sq_recv = pl.pallas_call(
        functools.partial(exchange_kernel, n, rest),
        out_shape=(
            pltpu.VMEM((span - TILE_S, virtuals, pairs), jnp.float32),
            pltpu.VMEM((groups, pairs, span + TILE_S, LANES), jnp.float32),
            pltpu.VMEM((span * rest, pairs), jnp.float32),
            pltpu.VMEM((n, 1, pairs), jnp.float32),
        ),
        in_specs=[anywhere] * 5,
        out_specs=(vmem,) * 4,
        scratch_shapes=[
            pltpu.SMEM(tile_order.shape, jnp.int32),
            pltpu.VMEM((2, pairs), jnp.int32),
            pltpu.VMEM((1, occupied_energy.shape[0]), jnp.float32),
            pltpu.VMEM((pairs, LANES), jnp.float32),
            pltpu.VMEM((basis, virtuals), jnp.float32),
            pltpu.VMEM((pair_rows, basis, columns), jnp.float32),
            pltpu.VMEM((columns, deep), jnp.float32),
            pltpu.VMEM((columns // PARTS, 3 * deep), jnp.bfloat16),
            pltpu.VMEM((3 * deep, broad), jnp.bfloat16),
            pltpu.VMEM((pair_rows, LANES), jnp.float32),
            pltpu.VMEM((pair_rows, TILE_S, LANES), jnp.float32),
            pltpu.VMEM((n, groups, pair_rows, span, LANES), jnp.float32),
            pltpu.VMEM((columns * pair_rows, LANES), jnp.float32),
            pltpu.VMEM((n, pair_rows, span * rest), jnp.float32),
            pltpu.VMEM((1, pairs), jnp.float32),
            pltpu.VMEM((pairs, span * rest), jnp.float32),
            pltpu.SemaphoreType.DMA((3,)),
            pltpu.SemaphoreType.DMA((1,)),
            pltpu.SemaphoreType.DMA((1,)),
            pltpu.SemaphoreType.DMA((count,)),
            pltpu.SemaphoreType.DMA((count,)),
            pltpu.SemaphoreType.DMA((2,)),
        ],
        compiler_params=pltpu.CompilerParams(
            collective_id=0, has_side_effects=True, vmem_limit_bytes=42 * 1024 * 1024
        ),
        cost_estimate=pl.CostEstimate(flops=flops, bytes_accessed=4 * half_integrals.size, transcendentals=0),
        name="exchange",
    )(
        hbm(tile_order), hbm(pair_list.T), hbm(occupied_energy.reshape(1, -1)),
        hbm(jnp.swapaxes(half_integrals, 1, 2)), hbm(virtual_orbitals),
    )
    out, rms = pl.pallas_call(
        functools.partial(finish_kernel, columns * virtuals),
        out_shape=(
            jax.ShapeDtypeStruct((span, virtuals, pairs), jnp.float32),
            jax.ShapeDtypeStruct((1, pairs), jnp.float32),
        ),
        in_specs=[vmem] * 4,
        out_specs=(pl.BlockSpec(memory_space=pltpu.HBM),) * 2,
        scratch_shapes=[
            pltpu.VMEM((TILE_S, virtuals, pairs), jnp.float32),
            pltpu.VMEM((1, pairs), jnp.float32),
            pltpu.SemaphoreType.DMA((3,)),
        ],
        compiler_params=pltpu.CompilerParams(vmem_limit_bytes=8 * 1024 * 1024),
        name="finish",
    )(main, recv_main, rest_turned, sq_recv)
    return (jnp.transpose(out, (2, 0, 1)), rms.reshape(-1))


def solution(mesh):
    in_specs = (
        P(("groups", "wide"), None, None),
        P("groups", None),
        P("groups"),
        P("groups", None),
        P(),
    )
    out_specs = (P("groups", "wide", None), P("groups"))
    return jax.shard_map(
        functools.partial(shards, mesh.shape["wide"]),
        mesh=mesh, in_specs=in_specs, out_specs=out_specs, check_vma=False,
    )
```
